8 devices in a mesh: data: 1 (over z), pipe: 8 (over y, x, core).
Axes of the slice: x: 2, y: 2, z: 1, core: 2. Of those that a mesh axis runs over, the one named last changes fastest.
Arguments:
- x_slice: bfloat16 [2048, 2048], P(('data', 'pipe'))
- slice_idx: int32 [8], P(('data', 'pipe'))
- k_cache: bfloat16 [30720, 24, 128], P(('data', 'pipe'))
- v_cache: bfloat16 [30720, 24, 128], P(('data', 'pipe'))
- w_q: bfloat16 [8, 2048, 3072], P('pipe')
- w_kv: bfloat16 [8, 2048, 6144], P('pipe')
- w_o: bfloat16 [8, 3072, 2048], P('pipe')
- w_gate: bfloat16 [8, 2048, 8192], P('pipe')
- w_up: bfloat16 [8, 2048, 8192], P('pipe')
- w_down: bfloat16 [8, 8192, 2048], P('pipe')
Outputs:
- output 1: bfloat16 [2048, 2048], P(('data', 'pipe'))
- output 2: float32 [2048, 24], P(('data', 'pipe'))
All inputs are finite; a program needn't handle non-finite values.
Results may differ from the reference program's by a relative error of at most 0.00906081.
Values are sent between devices in bfloat16 or wider.
A program may use at most 1 GiB of HBM per device.

```python
import jax
import jax.numpy as jnp
from jax import lax

STAGES = 8
D_MODEL = 2048
N_HEADS = 24
HEAD_DIM = 128
D_FF = 8192
SLICE_LEN = 256
N_SLICES = 16
P_MAX = 3840
QKV_WIDTH = N_HEADS * HEAD_DIM


def setup_inputs(seed: int = 0, part: int = 0) -> dict:
    shared = jax.random.split(jax.random.key(seed), 8)
    part_keys = jax.random.split(jax.random.fold_in(shared[6], part), 4)
    tick_base = jax.random.randint(shared[7], (), 0, N_SLICES)
    tick_num = (tick_base + part) % N_SLICES
    slice_idx = ((tick_num - jnp.arange(STAGES)) % N_SLICES).astype(jnp.int32)

    def normal_draw(rng_key, dims_shape, spread):
        return (jax.random.normal(rng_key, dims_shape, jnp.float32) * spread).astype(jnp.bfloat16)

    return {
        'x_slice': normal_draw(part_keys[1], (STAGES * SLICE_LEN, D_MODEL), 1.0),
        'slice_idx': slice_idx,
        'k_cache': normal_draw(part_keys[2], (STAGES * P_MAX, N_HEADS, HEAD_DIM), 1.0),
        'v_cache': normal_draw(part_keys[3], (STAGES * P_MAX, N_HEADS, HEAD_DIM), 1.0),
        'w_q': normal_draw(shared[0], (STAGES, D_MODEL, QKV_WIDTH), 2.0 * D_MODEL ** -0.5),
        'w_kv': normal_draw(shared[1], (STAGES, D_MODEL, 2 * QKV_WIDTH), D_MODEL ** -0.5),
        'w_o': normal_draw(shared[2], (STAGES, QKV_WIDTH, D_MODEL), 2.0 * QKV_WIDTH ** -0.5),
        'w_gate': normal_draw(shared[3], (STAGES, D_MODEL, D_FF), D_MODEL ** -0.5),
        'w_up': normal_draw(shared[4], (STAGES, D_MODEL, D_FF), D_MODEL ** -0.5),
        'w_down': normal_draw(shared[5], (STAGES, D_FF, D_MODEL), D_FF ** -0.5),
    }


def rms_normalize(values):
    stats_f32 = values.astype(jnp.float32)
    inv_rms = lax.rsqrt(jnp.mean(stats_f32 * stats_f32, axis=-1, keepdims=True) + 1e-6)
    return (stats_f32 * inv_rms).astype(jnp.bfloat16)


def stage_layer(stage_ops):
    x_stage, stage_blocks, k_stage, v_stage, wq_stage, wkv_stage, wo_stage, wg_stage, wu_stage, wd_stage = stage_ops
    normed = rms_normalize(x_stage)
    q_heads = jnp.dot(normed, wq_stage, preferred_element_type=jnp.float32).astype(jnp.bfloat16).reshape(SLICE_LEN, N_HEADS, HEAD_DIM)
    kv_new = jnp.dot(normed, wkv_stage, preferred_element_type=jnp.float32).astype(jnp.bfloat16)
    k_all = jnp.concatenate([k_stage, kv_new[:, :QKV_WIDTH].reshape(SLICE_LEN, N_HEADS, HEAD_DIM)], axis=0)
    v_all = jnp.concatenate([v_stage, kv_new[:, QKV_WIDTH:].reshape(SLICE_LEN, N_HEADS, HEAD_DIM)], axis=0)
    key_pos = jnp.arange(P_MAX + SLICE_LEN)[None, :]
    query_pos = jnp.arange(SLICE_LEN)[:, None]
    visible = jnp.where(key_pos < P_MAX, key_pos < stage_blocks * SLICE_LEN, key_pos - P_MAX <= query_pos)
    attn_scale = HEAD_DIM ** -0.5

    def head_attend(head_ops):
        q_one, k_one, v_one = head_ops
        scores = jnp.dot(q_one, k_one.T, preferred_element_type=jnp.float32) * attn_scale
        scores = jnp.where(visible, scores, -1e30)
        row_peak = jnp.max(scores, axis=-1, keepdims=True)
        log_sum = row_peak + jnp.log(jnp.sum(jnp.exp(scores - row_peak), axis=-1, keepdims=True))
        prob_bf16 = jnp.exp(scores - log_sum).astype(jnp.bfloat16)
        return jnp.dot(prob_bf16, v_one, preferred_element_type=jnp.float32), log_sum[:, 0]

    head_out, head_lse = lax.map(head_attend, (q_heads.transpose(1, 0, 2), k_all.transpose(1, 0, 2), v_all.transpose(1, 0, 2)))
    attn_out = head_out.transpose(1, 0, 2).reshape(SLICE_LEN, QKV_WIDTH).astype(jnp.bfloat16)
    resid_out = (x_stage.astype(jnp.float32) + jnp.dot(attn_out, wo_stage, preferred_element_type=jnp.float32)).astype(jnp.bfloat16)
    mlp_in = rms_normalize(resid_out)
    gate_act = jnp.dot(mlp_in, wg_stage, preferred_element_type=jnp.float32)
    up_act = jnp.dot(mlp_in, wu_stage, preferred_element_type=jnp.float32)
    hidden = (jax.nn.silu(gate_act) * up_act).astype(jnp.bfloat16)
    y_stage = (resid_out.astype(jnp.float32) + jnp.dot(hidden, wd_stage, preferred_element_type=jnp.float32)).astype(jnp.bfloat16)
    return y_stage, head_lse.T


def reference(x_slice, slice_idx, k_cache, v_cache, w_q, w_kv, w_o, w_gate, w_up, w_down):
    stage_ops = (
        x_slice.reshape(STAGES, SLICE_LEN, D_MODEL),
        slice_idx,
        k_cache.reshape(STAGES, P_MAX, N_HEADS, HEAD_DIM),
        v_cache.reshape(STAGES, P_MAX, N_HEADS, HEAD_DIM),
        w_q, w_kv, w_o, w_gate, w_up, w_down,
    )
    y_stages, lse_stages = lax.map(stage_layer, stage_ops)
    y_next = jnp.roll(y_stages, 1, axis=0).reshape(STAGES * SLICE_LEN, D_MODEL)
    return y_next, lse_stages.reshape(STAGES * SLICE_LEN, N_HEADS)
```

```python
import math

import jax
import jax.numpy as jnp
from jax import lax
from jax.experimental import pallas as pl
from jax.experimental.pallas import tpu as pltpu
from jax.sharding import PartitionSpec as P

BF = jnp.bfloat16
F32 = jnp.float32
HD = 128
FLOOR = -1e30
VM = pl.BlockSpec(memory_space=pltpu.VMEM)
HBM = pl.BlockSpec(memory_space=pltpu.HBM)
SM = pl.BlockSpec(memory_space=pltpu.SMEM)


def rms(values):
    v = values.astype(F32)
    return (v * lax.rsqrt(jnp.mean(v * v, axis=-1, keepdims=True) + 1e-6)).astype(BF)


def qkv_kernel(q_steps, x_ref, wq_ref, wkv_ref, qt_ref, kv_ref, a_ref):
    i = pl.program_id(0)

    @pl.when(i == 0)
    def _():
        a_ref[...] = rms(x_ref[...])

    @pl.when(i < q_steps)
    def _():
        t = jnp.dot(a_ref[...], wq_ref[...], preferred_element_type=F32).astype(BF)
        for h in range(qt_ref.shape[0]):
            qt_ref[h] = t[:, h * HD:(h + 1) * HD].T

    @pl.when(i >= q_steps)
    def _():
        t = jnp.dot(a_ref[...], wkv_ref[...], preferred_element_type=F32).astype(BF)
        for h in range(kv_ref.shape[0]):
            kv_ref[h] = t[:, h * HD:(h + 1) * HD]


def qkv_call(x, w_q, w_kv, tile=512):
    rows, dm = x.shape
    width = w_q.shape[1]
    qs, hs = width // tile, tile // HD
    return pl.pallas_call(
        lambda *r: qkv_kernel(qs, *r),
        grid=(3 * qs,),
        in_specs=[
            pl.BlockSpec((rows, dm), lambda i: (0, 0)),
            pl.BlockSpec((dm, tile), lambda i: (0, jnp.minimum(i, qs - 1))),
            pl.BlockSpec((dm, tile), lambda i: (0, jnp.maximum(i - qs, 0))),
        ],
        out_specs=[
            pl.BlockSpec((hs, HD, rows), lambda i: (jnp.minimum(i, qs - 1), 0, 0)),
            pl.BlockSpec((hs, rows, HD), lambda i: (jnp.maximum(i - qs, 0), 0, 0)),
        ],
        out_shape=[
            jax.ShapeDtypeStruct((width // HD, HD, rows), BF),
            jax.ShapeDtypeStruct((2 * width // HD, rows, HD), BF),
        ],
        scratch_shapes=[pltpu.VMEM((rows, dm), BF)],
        compiler_params=pltpu.CompilerParams(vmem_limit_bytes=60 * 2**20),
    )(x, w_q, w_kv)


G = 3


def attn_kernel(idx_ref, qt_ref, kv_ref, k_hbm, v_hbm, o_ref, lse_ref, kraw, vraw, kt, vt, acc, m_s, l_s, *rest):
    sb = [rest[0:G], rest[G:2 * G]]
    pb = [rest[2 * G:3 * G], rest[3 * G:4 * G]]
    ab = rest[4 * G:4 * G + 2]
    sems = rest[4 * G + 2]
    n = idx_ref[0]
    heads, _, rows = qt_ref.shape
    kb = kraw.shape[1]
    ni = heads // (2 * G)
    c = HD ** -0.5 * math.log2(math.e)

    def copies(b):
        s = lax.rem(b, 2)
        return [
            pltpu.make_async_copy(k_hbm.at[pl.ds(b * kb, kb)], kraw.at[s], sems.at[s, 0]),
            pltpu.make_async_copy(v_hbm.at[pl.ds(b * kb, kb)], vraw.at[s], sems.at[s, 1]),
        ]

    def start(b):
        for d in copies(b):
            d.start()

    @pl.when(n > 0)
    def _():
        start(0)

    @pl.when(n > 1)
    def _():
        start(1)

    vis = lax.broadcasted_iota(jnp.int32, (rows, rows), 0) <= lax.broadcasted_iota(jnp.int32, (rows, rows), 1)

    def local(h, _):
        s = jnp.dot(kv_ref[h], qt_ref[h], preferred_element_type=F32) * c
        s = jnp.where(vis, s, FLOOR)
        m = jnp.max(s, axis=0, keepdims=True)
        e = jnp.exp2(s - m)
        m_s[h] = m
        l_s[h] = jnp.sum(e, axis=0, keepdims=True)
        acc[h] = jnp.dot(kv_ref[heads + h].T, e.astype(BF), preferred_element_type=F32)
        return 0

    lax.fori_loop(0, heads, local, 0, unroll=4)

    def scores(h, j, g):
        sb[j][g][...] = jnp.dot(kt[h], qt_ref[h], preferred_element_type=F32)

    def soft(h, j, g):
        s = sb[j][g][...]
        mo = m_s[h]
        mn = jnp.maximum(mo, jnp.max(s, axis=0, keepdims=True) * c)
        al = jnp.exp2(mo - mn)
        e = jnp.exp2(s * c - mn)
        l_s[h] = l_s[h] * al + jnp.sum(e, axis=0, keepdims=True)
        m_s[h] = mn
        ab[j][g] = al
        pb[j][g][...] = e.astype(BF)

    def value(h, j, g):
        acc[h] = acc[h] * ab[j][g] + jnp.dot(vt[h].T, pb[j][g][...], preferred_element_type=F32)

    def block(b, _):
        s = lax.rem(b, 2)
        for d in copies(b):
            d.wait()
        kt[...] = jnp.swapaxes(kraw[s], 0, 1)
        vt[...] = jnp.swapaxes(vraw[s], 0, 1)

        @pl.when(b + 2 < n)
        def _():
            start(b + 2)

        for g in range(G):
            scores(g, 0, g)
        for g in range(G):
            scores(G + g, 1, g)
            soft(g, 0, g)

        def step(r, _):
            ha = 2 * G * (r + 1)
            for g in range(G):
                value(ha - 2 * G + g, 0, g)
                scores(ha + g, 0, g)
                soft(ha - G + g, 1, g)
            for g in range(G):
                value(ha - G + g, 1, g)
                scores(ha + G + g, 1, g)
                soft(ha + g, 0, g)
            return 0

        lax.fori_loop(0, ni - 1, step, 0)
        for g in range(G):
            value(heads - 2 * G + g, 0, g)
            soft(heads - G + g, 1, g)
        for g in range(G):
            value(heads - G + g, 1, g)
        return 0

    lax.fori_loop(0, n, block, 0)

    for h in range(heads):
        l = l_s[h]
        o_ref[:, h * HD:(h + 1) * HD] = (acc[h] * (1.0 / l)).T.astype(BF)
        lse_ref[pl.ds(h, 1)] = (m_s[h] + jnp.log2(l)) * math.log(2.0)


def attn_call(idx, qt, kvn, k, v, kb=256):
    heads, hd, rows = qt.shape
    return pl.pallas_call(
        attn_kernel,
        in_specs=[SM, VM, VM, HBM, HBM],
        out_specs=[VM, VM],
        out_shape=[jax.ShapeDtypeStruct((rows, heads * hd), BF), jax.ShapeDtypeStruct((heads, rows), F32)],
        scratch_shapes=[pltpu.VMEM((2, kb, heads, hd), BF)] * 2
        + [pltpu.VMEM((heads, kb, hd), BF)] * 2
        + [pltpu.VMEM((heads, hd, rows), F32), pltpu.VMEM((heads, 1, rows), F32), pltpu.VMEM((heads, 1, rows), F32)]
        + [pltpu.VMEM((kb, rows), F32)] * (2 * G)
        + [pltpu.VMEM((kb, rows), BF)] * (2 * G)
        + [pltpu.VMEM((G, 1, rows), F32)] * 2
        + [pltpu.SemaphoreType.DMA((2, 2))],
        compiler_params=pltpu.CompilerParams(vmem_limit_bytes=60 * 2**20),
    )(idx, qt, kvn, k, v)


def oproj_kernel(o_ref, x_ref, w_ref, h_ref, b_ref):
    i = pl.program_id(0)
    tile = w_ref.shape[1]
    cols = pl.ds(pl.multiple_of(i * tile, tile), tile)
    h_ref[:, cols] = (x_ref[...].astype(F32) + jnp.dot(o_ref[...], w_ref[...], preferred_element_type=F32)).astype(BF)

    @pl.when(i == pl.num_programs(0) - 1)
    def _():
        b_ref[...] = rms(h_ref[...])


def oproj_call(o, x, w, tile=512):
    rows, dm = x.shape
    return pl.pallas_call(
        oproj_kernel,
        grid=(dm // tile,),
        in_specs=[
            pl.BlockSpec(o.shape, lambda i: (0, 0)),
            pl.BlockSpec((rows, tile), lambda i: (0, i)),
            pl.BlockSpec((w.shape[0], tile), lambda i: (0, i)),
        ],
        out_specs=[pl.BlockSpec((rows, dm), lambda i: (0, 0))] * 2,
        out_shape=[jax.ShapeDtypeStruct((rows, dm), BF)] * 2,
        compiler_params=pltpu.CompilerParams(vmem_limit_bytes=60 * 2**20),
    )(o, x, w)


def glu_kernel(b_ref, g_ref, u_ref, o_ref):
    g = jnp.dot(b_ref[...], g_ref[...], preferred_element_type=F32)
    u = jnp.dot(b_ref[...], u_ref[...], preferred_element_type=F32)
    o_ref[...] = (jax.nn.silu(g) * u).astype(BF)


def glu_call(b, wg, wu, tile=512):
    rows, dm = b.shape
    ff = wg.shape[1]
    return pl.pallas_call(
        glu_kernel,
        grid=(ff // tile,),
        in_specs=[
            pl.BlockSpec((rows, dm), lambda i: (0, 0)),
            pl.BlockSpec((dm, tile), lambda i: (0, i)),
            pl.BlockSpec((dm, tile), lambda i: (0, i)),
        ],
        out_specs=pl.BlockSpec((rows, tile), lambda i: (0, i)),
        out_shape=jax.ShapeDtypeStruct((rows, ff), BF),
        compiler_params=pltpu.CompilerParams(vmem_limit_bytes=60 * 2**20),
    )(b, wg, wu)


def down_kernel(t_ref, h_ref, w_ref, y_ref):
    y_ref[...] = (h_ref[...].astype(F32) + jnp.dot(t_ref[...], w_ref[...], preferred_element_type=F32)).astype(BF)


def down_call(t, h, w, tile=256):
    rows, dm = h.shape
    return pl.pallas_call(
        down_kernel,
        grid=(dm // tile,),
        in_specs=[
            pl.BlockSpec(t.shape, lambda i: (0, 0)),
            pl.BlockSpec((rows, tile), lambda i: (0, i)),
            pl.BlockSpec((w.shape[0], tile), lambda i: (0, i)),
        ],
        out_specs=pl.BlockSpec((rows, tile), lambda i: (0, i)),
        out_shape=jax.ShapeDtypeStruct((rows, dm), BF),
        compiler_params=pltpu.CompilerParams(vmem_limit_bytes=60 * 2**20),
    )(t, h, w)


def solution(mesh):
    stages = mesh.shape['pipe']
    next_perm = [(s, (s + 1) % stages) for s in range(stages)]

    def device_step(x, idx, k, v, w_q, w_kv, w_o, w_gate, w_up, w_down):
        qt, kvn = qkv_call(x, w_q[0], w_kv[0])
        o, lse = attn_call(idx, qt, kvn, k, v)
        h, b = oproj_call(o, x, w_o[0])
        t = glu_call(b, w_gate[0], w_up[0])
        y = down_call(t, h, w_down[0])
        return lax.ppermute(y, 'pipe', next_perm), lse.T

    rows_spec = P(('data', 'pipe'), None)
    cache_spec = P(('data', 'pipe'), None, None)
    stage_spec = P('pipe', None, None)
    return jax.shard_map(
        device_step,
        mesh=mesh,
        in_specs=(rows_spec, P(('data', 'pipe')), cache_spec, cache_spec) + (stage_spec,) * 6,
        out_specs=(rows_spec, rows_spec),
        check_vma=False,
    )
```

```python
import math

import jax
import jax.numpy as jnp
from jax import lax
from jax.experimental import pallas as pl
from jax.experimental.pallas import tpu as pltpu
from jax.sharding import PartitionSpec as P

BF = jnp.bfloat16
F32 = jnp.float32
HD = 128
TN = 512
TK = 2048
RING = 12
RAW = 3
KB = 256
G = 4
FLOOR = -1e30
LIMIT = 2.0 ** 15
HBM = pl.BlockSpec(memory_space=pltpu.HBM)
SM = pl.BlockSpec(memory_space=pltpu.SMEM)


def rms(values):
    v = values.astype(F32)
    return (v * lax.rsqrt(jnp.mean(v * v, axis=-1, keepdims=True) + 1e-6)).astype(BF)


def dot(a, b):
    return jnp.dot(a, b, preferred_element_type=F32)


def layer_kernel(idx_ref, x_hbm, k_hbm, v_hbm, wq, wkv, wo, wg, wu, wd, y_hbm, lse_hbm,
                 ring, kraw, vraw, kt, vt, kn, vn, qa, acc, pb, mu_s, l_s, lb_s,
                 x_s, a_s, o_s, h_s, y_s, lse_s, wsem, ksem, msem):
    n = idx_ref[0]
    rows, dm = x_s.shape
    heads = qa.shape[0]
    c = HD ** -0.5 * math.log2(math.e)
    log2 = math.log(2.0)

    def col(i, w=TN):
        return pl.ds(pl.multiple_of(i * w, w), w)

    def fetch(e, src, height=TK):
        s = lax.rem(e, RING)
        pltpu.make_async_copy(src, ring.at[s, pl.ds(0, height)], wsem.at[s]).start()

    def ready(e, height=TK):
        s = lax.rem(e, RING)
        pltpu.make_async_copy(wg.at[pl.ds(0, height), pl.ds(0, TN)], ring.at[s, pl.ds(0, height)], wsem.at[s]).wait()
        return s

    def fetch_wo(e, nt):
        fetch(e, wo.at[pl.ds(0, TK), col(nt)])
        fetch(e + 1, wo.at[pl.ds(TK, wo.shape[0] - TK), col(nt)], wo.shape[0] - TK)

    def fetch_gu(e, nt):
        fetch(e, wg.at[:, col(nt)])
        fetch(e + 1, wu.at[:, col(nt)])

    def fetch_wd(e, j):
        for d in range(2):
            jj = j + d
            fetch(e + d, wd.at[col(lax.rem(jj, 4), TK), col(lax.div(jj, 4))])

    xcopy = pltpu.make_async_copy(x_hbm, x_s, msem.at[0])
    xcopy.start()
    for e in range(6):
        fetch(e, wq.at[:, pl.ds(e * TN, TN)])
    for e in range(6, RING):
        fetch(e, wkv.at[:, pl.ds((e - 6) * TN, TN)])

    def kv_copies(b):
        s = lax.rem(b, RAW)
        return [
            pltpu.make_async_copy(k_hbm.at[pl.ds(b * KB, KB)], kraw.at[s], ksem.at[s, 0]),
            pltpu.make_async_copy(v_hbm.at[pl.ds(b * KB, KB)], vraw.at[s], ksem.at[s, 1]),
        ]

    def kv_start(b):
        @pl.when(b < n)
        def _():
            for d in kv_copies(b):
                d.start()

    qa[:, HD:] = jnp.zeros((heads, qa.shape[1] - HD, rows), BF)
    xcopy.wait()
    a_s[...] = rms(x_s[...])

    def q_step(i, _):
        for d in range(2):
            e = 2 * i + d
            s = ready(e)
            t = dot(a_s[...], ring[s]).astype(BF)
            for j in range(4):
                qa[4 * e + j, 0:HD] = t[:, j * HD:(j + 1) * HD].T
        for d in range(2):
            e = 2 * i + d
            fetch(e + RING, wkv.at[:, col(e + RING - 6)])
        return 0

    lax.fori_loop(0, 3, q_step, 0)
    for b in range(RAW):
        kv_start(b)

    def kv_tiles(e, dst, base):
        for d in range(2):
            s = ready(e + d)
            t = dot(a_s[...], ring[s]).astype(BF)
            for j in range(4):
                dst[base + 4 * d + j] = t[:, j * HD:(j + 1) * HD]

    def k_step(i, _):
        e = 6 + 2 * i
        kv_tiles(e, kn, 8 * i)
        fetch_wo(e + RING, i)
        return 0

    lax.fori_loop(0, 3, k_step, 0)
    kv_tiles(12, vn, 0)
    fetch_wo(24, 3)

    def v_step(i, _):
        e = 14 + 2 * i
        kv_tiles(e, vn, 8 * i + 8)
        fetch_gu(e + RING, i)
        return 0

    lax.fori_loop(0, 2, v_step, 0)

    def bf_round(v):
        return v.astype(BF).astype(F32)

    def set_shift(h, mu):
        mu_s[h] = mu
        first = lax.broadcasted_iota(jnp.int32, (16, rows), 0) == 0
        qa[h, HD:HD + 16] = jnp.where(first, -mu, 0.0).astype(BF)

    vis = lax.broadcasted_iota(jnp.int32, (KB, rows), 0) <= lax.broadcasted_iota(jnp.int32, (KB, rows), 1)

    def local(h, _):
        s = jnp.where(vis, dot(kn[h], qa[h, 0:HD]), FLOOR)
        mu = bf_round(jnp.max(s, axis=0, keepdims=True))
        e = jnp.exp2((s - mu) * c)
        l_s[h] = jnp.sum(e, axis=0, keepdims=True)
        acc[h] = dot(vn[h].T, e.astype(BF))
        set_shift(h, mu)
        return 0

    lax.fori_loop(0, heads, local, 0, unroll=4)

    def exact(h, par):
        s = dot(kt[h], qa[h, 0:HD])
        mo = mu_s[h]
        mu = jnp.maximum(mo, bf_round(jnp.max(s, axis=0, keepdims=True)))
        al = jnp.exp2((mo - mu) * c)
        e = jnp.exp2((s - mu) * c)
        l_s[h] = l_s[h] * al
        acc[h] = acc[h] * al
        lb_s[h] = jnp.sum(e, axis=0, keepdims=True)
        pb[par * heads + h] = e.astype(BF)
        set_shift(h, mu)

    def exact_all(par):
        def one(h, _):
            exact(h, par)
            return 0
        lax.fori_loop(0, heads, one, 0, unroll=2)

    ones = jnp.where(lax.broadcasted_iota(jnp.int32, (KB, HD), 1) == 0, 1.0, 0.0).astype(BF)

    def fast(h, par):
        s = dot(jnp.concatenate([kt[h], ones], axis=1), qa[h])
        e = jnp.exp2(s * c)
        pb[par * heads + h] = e.astype(BF)
        return jnp.sum(e, axis=0, keepdims=True)

    def value(h, par):
        l_s[h] = l_s[h] + lb_s[h]
        acc[h] = acc[h] + dot(vt[h].T, pb[par * heads + h])

    def take(raw, b, dst):
        dst[...] = jnp.swapaxes(raw[lax.rem(b, RAW)], 0, 1)

    @pl.when(n > 0)
    def _():
        for d in kv_copies(0):
            d.wait()
        take(kraw, 0, kt)
        exact_all(0)
        take(vraw, 0, vt)
        kv_start(RAW)

        def block(b, _):
            for d in kv_copies(b):
                d.wait()
            take(kraw, b, kt)
            par = lax.rem(b, 2)

            def group(i, _):
                for g in range(G):
                    value(G * i + g, 1 - par)
                for g in range(G):
                    lb_s[G * i + g] = fast(G * i + g, par)
                return 0

            lax.fori_loop(0, heads // G, group, 0)

            @pl.when(jnp.logical_not(jnp.max(lb_s[...]) <= LIMIT))
            def _():
                exact_all(par)

            take(vraw, b, vt)
            kv_start(b + RAW)
            return 0

        lax.fori_loop(1, n, block, 0)
        last = lax.rem(n - 1, 2)

        def tail(i, _):
            for g in range(G):
                value(G * i + g, last)
            return 0

        lax.fori_loop(0, heads // G, tail, 0)

    for h in range(heads):
        l = l_s[h]
        o_s[:, h * HD:(h + 1) * HD] = (acc[h] * (1.0 / l)).T.astype(BF)
        lse_s[pl.ds(h, 1)] = mu_s[h] * (HD ** -0.5) + jnp.log2(l) * log2
    lcopy = pltpu.make_async_copy(lse_s, lse_hbm, msem.at[1])
    lcopy.start()

    def o_step(nt, _):
        e = 18 + 2 * nt
        s0 = ready(e)
        s1 = ready(e + 1, wo.shape[0] - TK)
        r = dot(o_s[:, 0:TK], ring[s0]) + dot(o_s[:, TK:], ring[s1, pl.ds(0, wo.shape[0] - TK)])
        h_s[:, col(nt)] = (x_s[:, col(nt)].astype(F32) + r).astype(BF)
        fetch_gu(e + RING, nt + 2)
        return 0

    lax.fori_loop(0, 4, o_step, 0)
    a_s[...] = rms(h_s[...])

    def gu_tile(nt):
        s0 = ready(26 + 2 * nt)
        s1 = ready(27 + 2 * nt)
        g = dot(a_s[...], ring[s0])
        u = dot(a_s[...], ring[s1])
        t = (jax.nn.silu(g) * u).astype(BF)
        pb[2 * nt] = t[:, 0:256]
        pb[2 * nt + 1] = t[:, 256:512]

    def gu1(nt, _):
        gu_tile(nt)
        fetch_gu(26 + 2 * nt + RING, nt + 6)
        return 0

    def gu2(nt, _):
        gu_tile(nt)
        fetch_wd(26 + 2 * nt + RING, 2 * (nt - 10))
        return 0

    lax.fori_loop(0, 10, gu1, 0)
    lax.fori_loop(10, 16, gu2, 0)

    def down(nt):
        e = 58 + 4 * nt
        r = h_s[:, col(nt)].astype(F32)
        for kk in range(4):
            s = ready(e + kk)
            lhs = jnp.concatenate([pb[8 * kk + j] for j in range(8)], axis=1)
            r = r + dot(lhs, ring[s])
        y_s[:, col(nt)] = r.astype(BF)
        pltpu.make_async_copy(y_s.at[:, col(nt)], y_hbm.at[:, col(nt)], msem.at[2 + nt]).start()

    down(0)
    fetch_wd(70, 12)
    fetch_wd(72, 14)

    def down_step(nt, _):
        down(nt)
        return 0

    lax.fori_loop(1, 4, down_step, 0)
    lcopy.wait()
    for nt in range(4):
        pltpu.make_async_copy(y_s.at[:, pl.ds(nt * TN, TN)], y_hbm.at[:, pl.ds(nt * TN, TN)], msem.at[2 + nt]).wait()


def layer_call(idx, x, k, v, wq, wkv, wo, wg, wu, wd):
    rows, dm = x.shape
    heads, hd = k.shape[1:]
    vm = pltpu.VMEM
    return pl.pallas_call(
        layer_kernel,
        in_specs=[SM] + [HBM] * 9,
        out_specs=[HBM, HBM],
        out_shape=[jax.ShapeDtypeStruct((rows, dm), BF), jax.ShapeDtypeStruct((heads, rows), F32)],
        scratch_shapes=[
            vm((RING, TK, TN), BF),
            vm((RAW, KB, heads, hd), BF),
            vm((RAW, KB, heads, hd), BF),
            vm((heads, KB, hd), BF),
            vm((heads, KB, hd), BF),
            vm((heads, rows, hd), BF),
            vm((heads, rows, hd), BF),
            vm((heads, 2 * hd, rows), BF),
            vm((heads, hd, rows), F32),
            vm((2 * heads, KB, rows), BF),
            vm((heads, 1, rows), F32),
            vm((heads, 1, rows), F32),
            vm((heads, 1, rows), F32),
            vm((rows, dm), BF),
            vm((rows, dm), BF),
            vm((rows, heads * hd), BF),
            vm((rows, dm), BF),
            vm((rows, dm), BF),
            vm((heads, rows), F32),
            pltpu.SemaphoreType.DMA((RING,)),
            pltpu.SemaphoreType.DMA((RAW, 2)),
            pltpu.SemaphoreType.DMA((6,)),
        ],
        compiler_params=pltpu.CompilerParams(vmem_limit_bytes=67043328),
    )(idx, x, k, v, wq, wkv, wo, wg, wu, wd)


def solution(mesh):
    stages = mesh.shape['pipe']
    next_perm = [(s, (s + 1) % stages) for s in range(stages)]

    def device_step(x, idx, k, v, w_q, w_kv, w_o, w_gate, w_up, w_down):
        y, lse = layer_call(idx, x, k, v, w_q[0], w_kv[0], w_o[0], w_gate[0], w_up[0], w_down[0])
        return lax.ppermute(y, 'pipe', next_perm), lse.T

    rows_spec = P(('data', 'pipe'), None)
    cache_spec = P(('data', 'pipe'), None, None)
    stage_spec = P('pipe', None, None)
    return jax.shard_map(
        device_step,
        mesh=mesh,
        in_specs=(rows_spec, P(('data', 'pipe')), cache_spec, cache_spec) + (stage_spec,) * 6,
        out_specs=(rows_spec, rows_spec),
        check_vma=False,
    )
```

```python
import math

import jax
import jax.numpy as jnp
from jax import lax
from jax.experimental import pallas as pl
from jax.experimental.pallas import tpu as pltpu
from jax.sharding import PartitionSpec as P

BF = jnp.bfloat16
F32 = jnp.float32
HD = 128
TN = 512
TK = 2048
RING = 12
KRAW = 3
VRAW = 4
KB = 256
FLOOR = -1e30
LIMIT = 2.0 ** 15
HBM = pl.BlockSpec(memory_space=pltpu.HBM)
SM = pl.BlockSpec(memory_space=pltpu.SMEM)


def rms(values):
    v = values.astype(F32)
    return (v * lax.rsqrt(jnp.mean(v * v, axis=-1, keepdims=True) + 1e-6)).astype(BF)


def dot(a, b):
    return jnp.dot(a, b, preferred_element_type=F32)


def layer_kernel(idx_ref, x_hbm, k_hbm, v_hbm, wq, wkv, wo, wg, wu, t_hbm, h_hbm, lse_hbm,
                 ring, kraw, vraw, kt, kn, vn, qa, acc, pb, mu_s, l_s, lb_s,
                 x_s, a_s, o_s, h_s, t_s, lse_s, wsem, ksem, msem, tsem):
    n = idx_ref[0]
    rows, dm = x_s.shape
    heads = qa.shape[0]
    c = HD ** -0.5 * math.log2(math.e)
    log2 = math.log(2.0)

    def col(i, w=TN):
        return pl.ds(pl.multiple_of(i * w, w), w)

    def fetch(e, src, height=TK):
        s = lax.rem(e, RING)
        pltpu.make_async_copy(src, ring.at[s, pl.ds(0, height)], wsem.at[s]).start()

    def ready(e, height=TK):
        s = lax.rem(e, RING)
        pltpu.make_async_copy(wg.at[pl.ds(0, height), pl.ds(0, TN)], ring.at[s, pl.ds(0, height)], wsem.at[s]).wait()
        return s

    def fetch_wo(e, nt):
        fetch(e, wo.at[pl.ds(0, TK), col(nt)])
        fetch(e + 1, wo.at[pl.ds(TK, wo.shape[0] - TK), col(nt)], wo.shape[0] - TK)

    def fetch_gu(e, nt):
        fetch(e, wg.at[:, col(nt)])
        fetch(e + 1, wu.at[:, col(nt)])

    xcopy = pltpu.make_async_copy(x_hbm, x_s, msem.at[0])
    xcopy.start()
    for e in range(6):
        fetch(e, wq.at[:, pl.ds(e * TN, TN)])
    for e in range(6, RING):
        fetch(e, wkv.at[:, pl.ds((e - 6) * TN, TN)])

    def kv_copies(b):
        s, t = lax.rem(b, KRAW), lax.rem(b, VRAW)
        return [
            pltpu.make_async_copy(k_hbm.at[pl.ds(b * KB, KB)], kraw.at[s], ksem.at[0, s]),
            pltpu.make_async_copy(v_hbm.at[pl.ds(b * KB, KB)], vraw.at[t], ksem.at[1, t]),
        ]

    def kv_start(b):
        @pl.when(b < n)
        def _():
            for d in kv_copies(b):
                d.start()

    qa[:, HD:] = jnp.zeros((heads, qa.shape[1] - HD, rows), BF)
    xcopy.wait()
    a_s[...] = rms(x_s[...])

    def q_step(i, _):
        for d in range(2):
            e = 2 * i + d
            s = ready(e)
            t = dot(a_s[...], ring[s]).astype(BF)
            for j in range(4):
                qa[4 * e + j, 0:HD] = t[:, j * HD:(j + 1) * HD].T
        for d in range(2):
            e = 2 * i + d
            fetch(e + RING, wkv.at[:, col(e + RING - 6)])
        return 0

    lax.fori_loop(0, 3, q_step, 0)
    kv_start(0)
    kv_start(1)

    def kv_tiles(e, dst, base):
        for d in range(2):
            s = ready(e + d)
            t = dot(a_s[...], ring[s]).astype(BF)
            for j in range(4):
                dst[base + 4 * d + j] = t[:, j * HD:(j + 1) * HD]

    def k_step(i, _):
        e = 6 + 2 * i
        kv_tiles(e, kn, 8 * i)
        fetch_wo(e + RING, i)
        return 0

    lax.fori_loop(0, 3, k_step, 0)
    kv_tiles(12, vn, 0)
    fetch_wo(24, 3)

    def v_step(i, _):
        e = 14 + 2 * i
        kv_tiles(e, vn, 8 * i + 8)
        fetch_gu(e + RING, i)
        return 0

    lax.fori_loop(0, 2, v_step, 0)

    def bf_round(v):
        return v.astype(BF).astype(F32)

    def set_shift(h, mu):
        mu_s[h] = mu
        first = lax.broadcasted_iota(jnp.int32, (16, rows), 0) == 0
        qa[h, HD:HD + 16] = jnp.where(first, -mu, 0.0).astype(BF)

    vis = lax.broadcasted_iota(jnp.int32, (KB, rows), 0) <= lax.broadcasted_iota(jnp.int32, (KB, rows), 1)

    def local(h, _):
        s = jnp.where(vis, dot(kn[h], qa[h, 0:HD]), FLOOR)
        mu = bf_round(jnp.max(s, axis=0, keepdims=True))
        e = jnp.exp2((s - mu) * c)
        l_s[h] = jnp.sum(e, axis=0, keepdims=True)
        acc[h] = dot(vn[h].T, e.astype(BF))
        set_shift(h, mu)
        return 0

    @pl.when(n == 0)
    def _():
        lax.fori_loop(0, heads, local, 0, unroll=4)

    def exact(h, par):
        s = dot(kt[h], qa[h, 0:HD])
        mo = mu_s[h]
        mu = jnp.maximum(mo, bf_round(jnp.max(s, axis=0, keepdims=True)))
        al = jnp.exp2((mo - mu) * c)
        e = jnp.exp2((s - mu) * c)
        l_s[h] = l_s[h] * al
        acc[h] = acc[h] * al
        lb_s[h] = jnp.sum(e, axis=0, keepdims=True)
        pb[par * heads + h] = e.astype(BF)
        set_shift(h, mu)

    def exact_all(b, par):
        kt[...] = jnp.swapaxes(kraw[lax.rem(b, KRAW)], 0, 1)

        def one(h, _):
            exact(h, par)
            return 0
        lax.fori_loop(0, heads, one, 0, unroll=2)

    ones = jnp.where(lax.broadcasted_iota(jnp.int32, (KB, HD), 1) == 0, 1.0, 0.0).astype(BF)
    k2 = kraw.reshape(KRAW, KB * heads, HD)
    v2 = vraw.reshape(VRAW, KB * heads, HD)

    def fast(h, par, slot):
        k = k2.at[slot][pl.ds(h, KB, stride=heads), :]
        e = jnp.exp2(dot(jnp.concatenate([k, ones], axis=1), qa[h]) * c)
        pb[par * heads + h] = e.astype(BF)
        lb_s[h] = jnp.sum(e, axis=0, keepdims=True)

    def value(h, par, slot):
        v = v2.at[slot][pl.ds(h, KB, stride=heads), :]
        l_s[h] = l_s[h] + lb_s[h]
        acc[h] = acc[h] + dot(v.T, pb[par * heads + h])

    def first(h):
        q = qa[h, 0:HD]
        s0 = jnp.where(vis, dot(kn[h], q), FLOOR)
        s1 = dot(k2.at[0][pl.ds(h, KB, stride=heads), :], q)
        mu = bf_round(jnp.maximum(jnp.max(s0, axis=0, keepdims=True), jnp.max(s1, axis=0, keepdims=True)))
        e0 = jnp.exp2((s0 - mu) * c)
        e1 = jnp.exp2((s1 - mu) * c)
        l_s[h] = jnp.sum(e0, axis=0, keepdims=True)
        lb_s[h] = jnp.sum(e1, axis=0, keepdims=True)
        pb[h] = e1.astype(BF)
        acc[h] = dot(vn[h].T, e0.astype(BF))
        set_shift(h, mu)

    @pl.when(n > 0)
    def _():
        for d in kv_copies(0):
            d.wait()
        kv_start(2)
        for h in range(heads):
            first(h)

        def block(b, _):
            for d in kv_copies(b):
                d.wait()
            kv_start(b + 2)
            par = lax.rem(b, 2)
            ks, vs = lax.rem(b, KRAW), lax.rem(b - 1, VRAW)
            for h in range(heads):
                value(h, 1 - par, vs)
                fast(h, par, ks)

            @pl.when(jnp.logical_not(jnp.max(lb_s[...]) <= LIMIT))
            def _():
                exact_all(b, par)

            return 0

        lax.fori_loop(1, n, block, 0)
        for h in range(heads):
            value(h, lax.rem(n - 1, 2), lax.rem(n - 1, VRAW))

    for h in range(heads):
        l = l_s[h]
        o_s[:, h * HD:(h + 1) * HD] = (acc[h] * (1.0 / l)).T.astype(BF)
        lse_s[pl.ds(h, 1)] = mu_s[h] * (HD ** -0.5) + jnp.log2(l) * log2
    lcopy = pltpu.make_async_copy(lse_s, lse_hbm, msem.at[1])
    lcopy.start()

    def o_step(nt, _):
        e = 18 + 2 * nt
        s0 = ready(e)
        s1 = ready(e + 1, wo.shape[0] - TK)
        r = dot(o_s[:, 0:TK], ring[s0]) + dot(o_s[:, TK:], ring[s1, pl.ds(0, wo.shape[0] - TK)])
        h_s[:, col(nt)] = (x_s[:, col(nt)].astype(F32) + r).astype(BF)
        fetch_gu(e + RING, nt + 2)
        return 0

    lax.fori_loop(0, 4, o_step, 0)
    a_s[...] = rms(h_s[...])

    hcopy = pltpu.make_async_copy(h_s, h_hbm, msem.at[2])
    hcopy.start()

    def t_copy(nt):
        return pltpu.make_async_copy(t_s.at[:, col(nt)], t_hbm.at[:, col(nt)], tsem.at[nt])

    def gu_tile(nt):
        s0 = ready(26 + 2 * nt)
        s1 = ready(27 + 2 * nt)
        g = dot(a_s[...], ring[s0])
        u = dot(a_s[...], ring[s1])
        t_s[:, col(nt)] = (jax.nn.silu(g) * u).astype(BF)
        t_copy(nt).start()

    def gu1(nt, _):
        gu_tile(nt)
        fetch_gu(26 + 2 * nt + RING, nt + 6)
        return 0

    def gu2(nt, _):
        gu_tile(nt)
        return 0

    def drain(nt, _):
        t_copy(nt).wait()
        return 0

    lax.fori_loop(0, 10, gu1, 0)
    lax.fori_loop(10, 16, gu2, 0)
    lcopy.wait()
    hcopy.wait()
    lax.fori_loop(0, 16, drain, 0)


def down_kernel(stages, t_hbm, h_hbm, wd, y_hbm, w_s, t_s, h_s, y_s, wsem, tsem, hsem, send, recv):
    me = lax.axis_index('pipe')
    nxt = lax.rem(me + 1, stages)
    prev = lax.rem(me + stages - 1, stages)
    chunks = w_s.shape[0]
    parts = t_s.shape[0]
    width = w_s.shape[2]
    depth = t_s.shape[2]
    barrier = pltpu.get_barrier_semaphore()
    pl.semaphore_signal(barrier, inc=1, device_id={'pipe': prev}, device_id_type=pl.DeviceIdType.MESH)

    def wcopy(i, k):
        return pltpu.make_async_copy(
            wd.at[pl.ds(k * depth, depth), pl.ds(i * width, width)], w_s.at[i, pl.ds(k * depth, depth)], wsem.at[i, k])

    tcopies = [pltpu.make_async_copy(t_hbm.at[:, pl.ds(k * depth, depth)], t_s.at[k], tsem.at[k]) for k in range(parts)]
    hcopy = pltpu.make_async_copy(h_hbm, h_s, hsem)
    for k in range(parts):
        tcopies[k].start()
        wcopy(0, k).start()
        if k == 0:
            hcopy.start()
    for i in range(1, chunks):
        for k in range(parts):
            wcopy(i, k).start()

    def out(i):
        cols = pl.ds(i * width, width)
        return pltpu.make_async_remote_copy(
            src_ref=y_s.at[:, cols], dst_ref=y_hbm.at[:, cols], send_sem=send.at[i], recv_sem=recv.at[i],
            device_id={'pipe': nxt}, device_id_type=pl.DeviceIdType.MESH)

    hcopy.wait()
    for i in range(chunks):
        cols = pl.ds(i * width, width)
        r = h_s[:, cols].astype(F32)
        for k in range(parts):
            if i == 0:
                tcopies[k].wait()
            wcopy(i, k).wait()
            r = r + dot(t_s[k], w_s[i, pl.ds(k * depth, depth)])
        y_s[:, cols] = r.astype(BF)
        if i == 0:
            pl.semaphore_wait(barrier, 1)
        out(i).start()
    for i in range(chunks):
        out(i).wait()


def down_call(t, h, wd, stages, width=256, parts=4):
    rows, dm = h.shape
    ff = t.shape[1]
    chunks = dm // width
    vm = pltpu.VMEM
    return pl.pallas_call(
        lambda *r: down_kernel(stages, *r),
        in_specs=[HBM] * 3,
        out_specs=HBM,
        out_shape=jax.ShapeDtypeStruct((rows, dm), BF),
        scratch_shapes=[
            vm((chunks, ff, width), BF),
            vm((parts, rows, ff // parts), BF),
            vm((rows, dm), BF),
            vm((rows, dm), BF),
            pltpu.SemaphoreType.DMA((chunks, parts)),
            pltpu.SemaphoreType.DMA((parts,)),
            pltpu.SemaphoreType.DMA,
            pltpu.SemaphoreType.DMA((chunks,)),
            pltpu.SemaphoreType.DMA((chunks,)),
        ],
        compiler_params=pltpu.CompilerParams(vmem_limit_bytes=60 * 2**20, collective_id=0, has_side_effects=True),
    )(t, h, wd)


def layer_call(idx, x, k, v, wq, wkv, wo, wg, wu, wd=None):
    rows, dm = x.shape
    ff = wg.shape[1]
    heads, hd = k.shape[1:]
    vm = pltpu.VMEM
    return pl.pallas_call(
        layer_kernel,
        in_specs=[SM] + [HBM] * 8,
        out_specs=[HBM] * 3,
        out_shape=[jax.ShapeDtypeStruct((rows, ff), BF), jax.ShapeDtypeStruct((rows, dm), BF), jax.ShapeDtypeStruct((heads, rows), F32)],
        scratch_shapes=[
            vm((RING, TK, TN), BF),
            vm((KRAW, KB, heads, hd), BF),
            vm((VRAW, KB, heads, hd), BF),
            vm((heads, KB, hd), BF),
            vm((heads, rows, hd), BF),
            vm((heads, rows, hd), BF),
            vm((heads, 2 * hd, rows), BF),
            vm((heads, hd, rows), F32),
            vm((2 * heads, KB, rows), BF),
            vm((heads, 1, rows), F32),
            vm((heads, 1, rows), F32),
            vm((heads, 1, rows), F32),
            vm((rows, dm), BF),
            vm((rows, dm), BF),
            vm((rows, heads * hd), BF),
            vm((rows, dm), BF),
            vm((rows, ff), BF),
            vm((heads, rows), F32),
            pltpu.SemaphoreType.DMA((RING,)),
            pltpu.SemaphoreType.DMA((2, VRAW)),
            pltpu.SemaphoreType.DMA((3,)),
            pltpu.SemaphoreType.DMA((16,)),
        ],
        compiler_params=pltpu.CompilerParams(vmem_limit_bytes=67043328),
    )(idx, x, k, v, wq, wkv, wo, wg, wu)


def solution(mesh):
    stages = mesh.shape['pipe']

    def device_step(x, idx, k, v, w_q, w_kv, w_o, w_gate, w_up, w_down):
        t, h, lse = layer_call(idx, x, k, v, w_q[0], w_kv[0], w_o[0], w_gate[0], w_up[0])
        return down_call(t, h, w_down[0], stages), lse.T

    rows_spec = P(('data', 'pipe'), None)
    cache_spec = P(('data', 'pipe'), None, None)
    stage_spec = P('pipe', None, None)
    return jax.shard_map(
        device_step,
        mesh=mesh,
        in_specs=(rows_spec, P(('data', 'pipe')), cache_spec, cache_spec) + (stage_spec,) * 6,
        out_specs=(rows_spec, rows_spec),
        check_vma=False,
    )
```

```python
import math

import jax
import jax.numpy as jnp
from jax import lax
from jax.experimental import pallas as pl
from jax.experimental.pallas import tpu as pltpu
from jax.sharding import PartitionSpec as P

BF = jnp.bfloat16
F32 = jnp.float32
HD = 128
TN = 512
TK = 2048
RING = 12
AHEAD = 4
KRAW = 3
VRAW = 4
KB = 256
FLOOR = -1e30
LIMIT = 2.0 ** 15
HBM = pl.BlockSpec(memory_space=pltpu.HBM)
SM = pl.BlockSpec(memory_space=pltpu.SMEM)


def rms(values):
    v = values.astype(F32)
    return (v * lax.rsqrt(jnp.mean(v * v, axis=-1, keepdims=True) + 1e-6)).astype(BF)


def dot(a, b):
    return jnp.dot(a, b, preferred_element_type=F32)


def layer_kernel(idx_ref, x_hbm, k_hbm, v_hbm, wq, wkv, wo, wg, wu, t_hbm, h_hbm, lse_hbm,
                 ring, kraw, vraw, kt, kn, vn, qa, acc, pb, mu_s, l_s, lb_s,
                 x_s, a_s, o_s, h_s, t_s, lse_s, wsem, ksem, msem, tsem):
    n = idx_ref[0]
    rows, dm = x_s.shape
    heads = qa.shape[0]
    c = HD ** -0.5 * math.log2(math.e)
    log2 = math.log(2.0)

    def col(i, w=TN):
        return pl.ds(pl.multiple_of(i * w, w), w)

    def fetch(e, src, height=TK):
        s = lax.rem(e, RING)
        pltpu.make_async_copy(src, ring.at[s, pl.ds(0, height)], wsem.at[s]).start()

    def ready(e, height=TK):
        s = lax.rem(e, RING)
        pltpu.make_async_copy(wg.at[pl.ds(0, height), pl.ds(0, TN)], ring.at[s, pl.ds(0, height)], wsem.at[s]).wait()
        return s

    def fetch_wo(e, nt):
        fetch(e, wo.at[pl.ds(0, TK), col(nt)])
        fetch(e + 1, wo.at[pl.ds(TK, wo.shape[0] - TK), col(nt)], wo.shape[0] - TK)

    def fetch_gu(e, nt):
        fetch(e, wg.at[:, col(nt)])
        fetch(e + 1, wu.at[:, col(nt)])

    def fetch_mid(e):
        rest = wo.shape[0] - TK
        even = lax.rem(e, 2) == 0
        nt = lax.div(e - 18, 2)

        @pl.when(jnp.logical_and(e < 26, even))
        def _():
            fetch(e, wo.at[pl.ds(0, TK), col(nt)])

        @pl.when(jnp.logical_and(e < 26, jnp.logical_not(even)))
        def _():
            fetch(e, wo.at[pl.ds(TK, rest), col(nt)], rest)

        @pl.when(jnp.logical_and(e >= 26, even))
        def _():
            fetch(e, wg.at[:, col(nt - 4)])

        @pl.when(jnp.logical_and(e >= 26, jnp.logical_not(even)))
        def _():
            fetch(e, wu.at[:, col(nt - 4)])

    xcopy = pltpu.make_async_copy(x_hbm, x_s, msem.at[0])
    xcopy.start()
    for e in range(AHEAD):
        fetch(e, wq.at[:, pl.ds(e * TN, TN)])

    def kv_copies(b):
        s, t = lax.rem(b, KRAW), lax.rem(b, VRAW)
        return [
            pltpu.make_async_copy(k_hbm.at[pl.ds(b * KB, KB)], kraw.at[s], ksem.at[0, s]),
            pltpu.make_async_copy(v_hbm.at[pl.ds(b * KB, KB)], vraw.at[t], ksem.at[1, t]),
        ]

    def kv_start(b):
        @pl.when(b < n)
        def _():
            for d in kv_copies(b):
                d.start()

    qa[:, HD:] = jnp.zeros((heads, qa.shape[1] - HD, rows), BF)
    xcopy.wait()
    a_s[...] = rms(x_s[...])

    def q_step(i, _):
        @pl.when(i == 0)
        def _():
            for d in range(AHEAD, 6):
                fetch(d, wq.at[:, pl.ds(d * TN, TN)])

        @pl.when(i > 0)
        def _():
            for d in range(2):
                fetch(2 * i + AHEAD + d, wkv.at[:, col(2 * i + AHEAD + d - 6)])

        for d in range(2):
            e = 2 * i + d
            s = ready(e)
            t = dot(a_s[...], ring[s]).astype(BF)
            for j in range(4):
                qa[4 * e + j, 0:HD] = t[:, j * HD:(j + 1) * HD].T
        return 0

    lax.fori_loop(0, 3, q_step, 0)

    def fetch_kv(e):
        for d in range(2):
            fetch(e + d, wkv.at[:, col(e + d - 6)])

    def kv_tiles(e, dst, base):
        for d in range(2):
            s = ready(e + d)
            t = dot(a_s[...], ring[s]).astype(BF)
            for j in range(4):
                dst[base + 4 * d + j] = t[:, j * HD:(j + 1) * HD]

    def k_step(i, _):
        e = 6 + 2 * i
        fetch_kv(e + AHEAD)
        kv_tiles(e, kn, 8 * i)
        return 0

    lax.fori_loop(0, 3, k_step, 0)
    fetch_kv(12 + AHEAD)
    kv_start(0)
    kv_start(1)
    kv_tiles(12, vn, 0)

    def v_step(i, _):
        e = 14 + 2 * i
        fetch_wo(e + AHEAD, i)
        kv_tiles(e, vn, 8 * i + 8)
        return 0

    lax.fori_loop(0, 2, v_step, 0)

    def bf_round(v):
        return v.astype(BF).astype(F32)

    def set_shift(h, mu):
        mu_s[h] = mu
        first = lax.broadcasted_iota(jnp.int32, (16, rows), 0) == 0
        qa[h, HD:HD + 16] = jnp.where(first, -mu, 0.0).astype(BF)

    vis = lax.broadcasted_iota(jnp.int32, (KB, rows), 0) <= lax.broadcasted_iota(jnp.int32, (KB, rows), 1)

    def local(h, _):
        s = jnp.where(vis, dot(kn[h], qa[h, 0:HD]), FLOOR)
        mu = bf_round(jnp.max(s, axis=0, keepdims=True))
        e = jnp.exp2((s - mu) * c)
        l_s[h] = jnp.sum(e, axis=0, keepdims=True)
        acc[h] = dot(vn[h].T, e.astype(BF))
        set_shift(h, mu)
        return 0

    @pl.when(n == 0)
    def _():
        lax.fori_loop(0, heads, local, 0, unroll=4)

    def exact(h, par):
        s = dot(kt[h], qa[h, 0:HD])
        mo = mu_s[h]
        mu = jnp.maximum(mo, bf_round(jnp.max(s, axis=0, keepdims=True)))
        al = jnp.exp2((mo - mu) * c)
        e = jnp.exp2((s - mu) * c)
        l_s[h] = l_s[h] * al
        acc[h] = acc[h] * al
        lb_s[h] = jnp.sum(e, axis=0, keepdims=True)
        pb[par * heads + h] = e.astype(BF)
        set_shift(h, mu)

    def exact_all(b, par):
        kt[...] = jnp.swapaxes(kraw[lax.rem(b, KRAW)], 0, 1)

        def one(h, _):
            exact(h, par)
            return 0
        lax.fori_loop(0, heads, one, 0, unroll=2)

    ones = jnp.where(lax.broadcasted_iota(jnp.int32, (KB, HD), 1) == 0, 1.0, 0.0).astype(BF)
    k2 = kraw.reshape(KRAW, KB * heads, HD)
    v2 = vraw.reshape(VRAW, KB * heads, HD)

    def fast(h, par, slot):
        k = k2.at[slot][pl.ds(h, KB, stride=heads), :]
        e = jnp.exp2(dot(jnp.concatenate([k, ones], axis=1), qa[h]) * c)
        pb[par * heads + h] = e.astype(BF)
        lb_s[h] = jnp.sum(e, axis=0, keepdims=True)

    def value(h, par, slot):
        v = v2.at[slot][pl.ds(h, KB, stride=heads), :]
        l_s[h] = l_s[h] + lb_s[h]
        acc[h] = acc[h] + dot(v.T, pb[par * heads + h])

    def first(h):
        q = qa[h, 0:HD]
        s0 = jnp.where(vis, dot(kn[h], q), FLOOR)
        s1 = dot(k2.at[0][pl.ds(h, KB, stride=heads), :], q)
        mu = bf_round(jnp.maximum(jnp.max(s0, axis=0, keepdims=True), jnp.max(s1, axis=0, keepdims=True)))
        e0 = jnp.exp2((s0 - mu) * c)
        e1 = jnp.exp2((s1 - mu) * c)
        l_s[h] = jnp.sum(e0, axis=0, keepdims=True)
        lb_s[h] = jnp.sum(e1, axis=0, keepdims=True)
        pb[h] = e1.astype(BF)
        acc[h] = dot(vn[h].T, e0.astype(BF))
        set_shift(h, mu)

    @pl.when(n > 0)
    def _():
        for d in kv_copies(0):
            d.wait()
        kv_start(2)
        for h in range(heads):
            first(h)

        def block(b, _):
            for d in kv_copies(b):
                d.wait()
            kv_start(b + 2)

            @pl.when(b <= 8)
            def _():
                fetch_mid(21 + b)

            par = lax.rem(b, 2)
            ks, vs = lax.rem(b, KRAW), lax.rem(b - 1, VRAW)
            for h in range(heads):
                value(h, 1 - par, vs)
                fast(h, par, ks)

            @pl.when(jnp.logical_not(jnp.max(lb_s[...]) <= LIMIT))
            def _():
                exact_all(b, par)

            return 0

        lax.fori_loop(1, n, block, 0)
        for h in range(heads):
            value(h, lax.rem(n - 1, 2), lax.rem(n - 1, VRAW))

    def late(e, _):
        fetch_mid(e)
        return 0

    lax.fori_loop(22 + jnp.clip(n - 1, 0, 8), 30, late, 0)
    for h in range(heads):
        l = l_s[h]
        o_s[:, h * HD:(h + 1) * HD] = (acc[h] * (1.0 / l)).T.astype(BF)
        lse_s[pl.ds(h, 1)] = mu_s[h] * (HD ** -0.5) + jnp.log2(l) * log2
    lcopy = pltpu.make_async_copy(lse_s, lse_hbm, msem.at[1])
    lcopy.start()

    def o_step(nt, _):
        e = 18 + 2 * nt
        s0 = ready(e)
        s1 = ready(e + 1, wo.shape[0] - TK)
        r = dot(o_s[:, 0:TK], ring[s0]) + dot(o_s[:, TK:], ring[s1, pl.ds(0, wo.shape[0] - TK)])
        h_s[:, col(nt)] = (x_s[:, col(nt)].astype(F32) + r).astype(BF)
        fetch_gu(e + RING, nt + 2)
        return 0

    lax.fori_loop(0, 4, o_step, 0)
    a_s[...] = rms(h_s[...])

    hcopy = pltpu.make_async_copy(h_s, h_hbm, msem.at[2])
    hcopy.start()

    def t_copy(nt):
        return pltpu.make_async_copy(t_s.at[:, col(nt)], t_hbm.at[:, col(nt)], tsem.at[nt])

    def gu_tile(nt):
        s0 = ready(26 + 2 * nt)
        s1 = ready(27 + 2 * nt)
        g = dot(a_s[...], ring[s0])
        u = dot(a_s[...], ring[s1])
        t_s[:, col(nt)] = (jax.nn.silu(g) * u).astype(BF)
        t_copy(nt).start()

    def gu1(nt, _):
        gu_tile(nt)
        fetch_gu(26 + 2 * nt + RING, nt + 6)
        return 0

    def gu2(nt, _):
        gu_tile(nt)
        return 0

    def drain(nt, _):
        t_copy(nt).wait()
        return 0

    lax.fori_loop(0, 10, gu1, 0)
    lax.fori_loop(10, 16, gu2, 0)
    lcopy.wait()
    hcopy.wait()
    lax.fori_loop(0, 16, drain, 0)


def down_kernel(stages, t_hbm, h_hbm, wd, y_hbm, w_s, t_s, h_s, y_s, wsem, tsem, hsem, send, recv):
    me = lax.axis_index('pipe')
    nxt = lax.rem(me + 1, stages)
    prev = lax.rem(me + stages - 1, stages)
    chunks = w_s.shape[0]
    parts = t_s.shape[0]
    width = w_s.shape[2]
    depth = t_s.shape[2]
    barrier = pltpu.get_barrier_semaphore()
    pl.semaphore_signal(barrier, inc=1, device_id={'pipe': prev}, device_id_type=pl.DeviceIdType.MESH)

    def wcopy(i, k):
        return pltpu.make_async_copy(
            wd.at[pl.ds(k * depth, depth), pl.ds(i * width, width)], w_s.at[i, pl.ds(k * depth, depth)], wsem.at[i, k])

    tcopies = [pltpu.make_async_copy(t_hbm.at[:, pl.ds(k * depth, depth)], t_s.at[k], tsem.at[k]) for k in range(parts)]
    hcopy = pltpu.make_async_copy(h_hbm, h_s, hsem)
    for k in range(parts):
        tcopies[k].start()
        wcopy(0, k).start()
        if k == 0:
            hcopy.start()
    ahead = 2
    for i in range(1, ahead):
        for k in range(parts):
            wcopy(i, k).start()

    def out(i):
        cols = pl.ds(i * width, width)
        return pltpu.make_async_remote_copy(
            src_ref=y_s.at[:, cols], dst_ref=y_hbm.at[:, cols], send_sem=send.at[i], recv_sem=recv.at[i],
            device_id={'pipe': nxt}, device_id_type=pl.DeviceIdType.MESH)

    hcopy.wait()
    for i in range(chunks):
        cols = pl.ds(i * width, width)
        for k in range(parts):
            if i == 0:
                tcopies[k].wait()
            wcopy(i, k).wait()
        if i + ahead < chunks:
            for k in range(parts):
                wcopy(i + ahead, k).start()
        r = h_s[:, cols].astype(F32) + dot(jnp.concatenate([t_s[k] for k in range(parts)], axis=1), w_s[i])
        y_s[:, cols] = r.astype(BF)
        if i == 0:
            pl.semaphore_wait(barrier, 1)
        out(i).start()
    for i in range(chunks):
        out(i).wait()


def down_call(t, h, wd, stages, width=256, parts=4):
    rows, dm = h.shape
    ff = t.shape[1]
    chunks = dm // width
    vm = pltpu.VMEM
    return pl.pallas_call(
        lambda *r: down_kernel(stages, *r),
        in_specs=[HBM] * 3,
        out_specs=pl.BlockSpec(memory_space=pltpu.VMEM),
        out_shape=jax.ShapeDtypeStruct((rows, dm), BF),
        scratch_shapes=[
            vm((chunks, ff, width), BF),
            vm((parts, rows, ff // parts), BF),
            vm((rows, dm), BF),
            vm((rows, dm), BF),
            pltpu.SemaphoreType.DMA((chunks, parts)),
            pltpu.SemaphoreType.DMA((parts,)),
            pltpu.SemaphoreType.DMA,
            pltpu.SemaphoreType.DMA((chunks,)),
            pltpu.SemaphoreType.DMA((chunks,)),
        ],
        compiler_params=pltpu.CompilerParams(vmem_limit_bytes=48 * 2**20, collective_id=0, has_side_effects=True),
    )(t, h, wd)


def layer_call(idx, x, k, v, wq, wkv, wo, wg, wu, wd=None):
    rows, dm = x.shape
    ff = wg.shape[1]
    heads, hd = k.shape[1:]
    vm = pltpu.VMEM
    return pl.pallas_call(
        layer_kernel,
        in_specs=[SM] + [HBM] * 8,
        out_specs=[HBM] * 3,
        out_shape=[jax.ShapeDtypeStruct((rows, ff), BF), jax.ShapeDtypeStruct((rows, dm), BF), jax.ShapeDtypeStruct((heads, rows), F32)],
        scratch_shapes=[
            vm((RING, TK, TN), BF),
            vm((KRAW, KB, heads, hd), BF),
            vm((VRAW, KB, heads, hd), BF),
            vm((heads, KB, hd), BF),
            vm((heads, rows, hd), BF),
            vm((heads, rows, hd), BF),
            vm((heads, 2 * hd, rows), BF),
            vm((heads, hd, rows), F32),
            vm((2 * heads, KB, rows), BF),
            vm((heads, 1, rows), F32),
            vm((heads, 1, rows), F32),
            vm((heads, 1, rows), F32),
            vm((rows, dm), BF),
            vm((rows, dm), BF),
            vm((rows, heads * hd), BF),
            vm((rows, dm), BF),
            vm((rows, ff), BF),
            vm((heads, rows), F32),
            pltpu.SemaphoreType.DMA((RING,)),
            pltpu.SemaphoreType.DMA((2, VRAW)),
            pltpu.SemaphoreType.DMA((3,)),
            pltpu.SemaphoreType.DMA((16,)),
        ],
        compiler_params=pltpu.CompilerParams(vmem_limit_bytes=67043328),
    )(idx, x, k, v, wq, wkv, wo, wg, wu)


def solution(mesh):
    stages = mesh.shape['pipe']

    def device_step(x, idx, k, v, w_q, w_kv, w_o, w_gate, w_up, w_down):
        t, h, lse = layer_call(idx, x, k, v, w_q[0], w_kv[0], w_o[0], w_gate[0], w_up[0])
        return down_call(t, h, w_down[0], stages), lse.T

    rows_spec = P(('data', 'pipe'), None)
    cache_spec = P(('data', 'pipe'), None, None)
    stage_spec = P('pipe', None, None)
    return jax.shard_map(
        device_step,
        mesh=mesh,
        in_specs=(rows_spec, P(('data', 'pipe')), cache_spec, cache_spec) + (stage_spec,) * 6,
        out_specs=(rows_spec, rows_spec),
        check_vma=False,
    )
```

```python
import math

import jax
import jax.numpy as jnp
from jax import lax
from jax.experimental import pallas as pl
from jax.experimental.pallas import tpu as pltpu
from jax.sharding import PartitionSpec as P

BF = jnp.bfloat16
F32 = jnp.float32
HD = 128
TN = 512
TK = 2048
RING = 12
AHEAD = 4
KRAW = 3
VRAW = 4
KB = 256
FLOOR = -1e30
LIMIT = 2.0 ** 15
HBM = pl.BlockSpec(memory_space=pltpu.HBM)
SM = pl.BlockSpec(memory_space=pltpu.SMEM)


def rms(values):
    v = values.astype(F32)
    return (v * lax.rsqrt(jnp.mean(v * v, axis=-1, keepdims=True) + 1e-6)).astype(BF)


def dot(a, b):
    return jnp.dot(a, b, preferred_element_type=F32)


def layer_kernel(idx_ref, x_hbm, k_hbm, v_hbm, wq, wkv, wo, wg, wu, t_hbm, h_hbm, lse_hbm,
                 ring, kraw, vraw, kt, kn, vn, qa, acc, pb, mu_s, l_s, lb_s,
                 x_s, a_s, o_s, h_s, t_s, lse_s, wsem, ksem, msem, tsem):
    n = idx_ref[0]
    rows, dm = x_s.shape
    heads = qa.shape[0]
    c = HD ** -0.5 * math.log2(math.e)
    log2 = math.log(2.0)

    def col(i, w=TN):
        return pl.ds(pl.multiple_of(i * w, w), w)

    def fetch(e, src, height=TK):
        s = lax.rem(e, RING)
        pltpu.make_async_copy(src, ring.at[s, pl.ds(0, height)], wsem.at[s]).start()

    def ready(e, height=TK):
        s = lax.rem(e, RING)
        pltpu.make_async_copy(wg.at[pl.ds(0, height), pl.ds(0, TN)], ring.at[s, pl.ds(0, height)], wsem.at[s]).wait()
        return s

    def fetch_wo(e, nt):
        fetch(e, wo.at[pl.ds(0, TK), col(nt)])
        fetch(e + 1, wo.at[pl.ds(TK, wo.shape[0] - TK), col(nt)], wo.shape[0] - TK)

    def fetch_gu(e, nt):
        fetch(e, wg.at[:, col(nt)])
        fetch(e + 1, wu.at[:, col(nt)])

    def fetch_mid(e):
        rest = wo.shape[0] - TK
        even = lax.rem(e, 2) == 0
        nt = lax.div(e - 18, 2)

        @pl.when(jnp.logical_and(e < 26, even))
        def _():
            fetch(e, wo.at[pl.ds(0, TK), col(nt)])

        @pl.when(jnp.logical_and(e < 26, jnp.logical_not(even)))
        def _():
            fetch(e, wo.at[pl.ds(TK, rest), col(nt)], rest)

        @pl.when(jnp.logical_and(e >= 26, even))
        def _():
            fetch(e, wg.at[:, col(nt - 4)])

        @pl.when(jnp.logical_and(e >= 26, jnp.logical_not(even)))
        def _():
            fetch(e, wu.at[:, col(nt - 4)])

    xcopy = pltpu.make_async_copy(x_hbm, x_s, msem.at[0])
    xcopy.start()
    for e in range(AHEAD):
        fetch(e, wq.at[:, pl.ds(e * TN, TN)])

    def kv_copies(b):
        s, t = lax.rem(b, KRAW), lax.rem(b, VRAW)
        return [
            pltpu.make_async_copy(k_hbm.at[pl.ds(b * KB, KB)], kraw.at[s], ksem.at[0, s]),
            pltpu.make_async_copy(v_hbm.at[pl.ds(b * KB, KB)], vraw.at[t], ksem.at[1, t]),
        ]

    def kv_start(b):
        @pl.when(b < n)
        def _():
            for d in kv_copies(b):
                d.start()

    qa[:, HD:] = jnp.zeros((heads, qa.shape[1] - HD, rows), BF)
    xcopy.wait()
    a_s[...] = rms(x_s[...])

    def q_step(i, _):
        @pl.when(i == 0)
        def _():
            for d in range(AHEAD, 6):
                fetch(d, wq.at[:, pl.ds(d * TN, TN)])

        @pl.when(i > 0)
        def _():
            for d in range(2):
                fetch(2 * i + AHEAD + d, wkv.at[:, col(2 * i + AHEAD + d - 6)])

        for d in range(2):
            e = 2 * i + d
            s = ready(e)
            t = dot(a_s[...], ring[s]).astype(BF)
            for j in range(4):
                qa[4 * e + j, 0:HD] = t[:, j * HD:(j + 1) * HD].T
        return 0

    lax.fori_loop(0, 3, q_step, 0)

    def fetch_kv(e):
        for d in range(2):
            fetch(e + d, wkv.at[:, col(e + d - 6)])

    def kv_tiles(e, dst, base):
        for d in range(2):
            s = ready(e + d)
            t = dot(a_s[...], ring[s]).astype(BF)
            for j in range(4):
                dst[base + 4 * d + j] = t[:, j * HD:(j + 1) * HD]

    def k_step(i, _):
        e = 6 + 2 * i
        fetch_kv(e + AHEAD)
        kv_tiles(e, kn, 8 * i)
        return 0

    lax.fori_loop(0, 3, k_step, 0)
    fetch_kv(12 + AHEAD)
    kv_start(0)
    kv_start(1)
    kv_tiles(12, vn, 0)

    def v_step(i, _):
        e = 14 + 2 * i
        fetch_wo(e + AHEAD, i)
        kv_tiles(e, vn, 8 * i + 8)
        return 0

    lax.fori_loop(0, 2, v_step, 0)

    def bf_round(v):
        return v.astype(BF).astype(F32)

    def set_shift(h, mu):
        mu_s[h] = mu
        first = lax.broadcasted_iota(jnp.int32, (16, rows), 0) == 0
        qa[h, HD:HD + 16] = jnp.where(first, -mu, 0.0).astype(BF)

    vis = lax.broadcasted_iota(jnp.int32, (KB, rows), 0) <= lax.broadcasted_iota(jnp.int32, (KB, rows), 1)

    def local(h, _):
        s = jnp.where(vis, dot(kn[h], qa[h, 0:HD]), FLOOR)
        mu = bf_round(jnp.max(s, axis=0, keepdims=True))
        e = jnp.exp2((s - mu) * c)
        l_s[h] = jnp.sum(e, axis=0, keepdims=True)
        acc[h] = dot(vn[h].T, e.astype(BF))
        set_shift(h, mu)
        return 0

    @pl.when(n == 0)
    def _():
        lax.fori_loop(0, heads, local, 0, unroll=4)

    def exact(h, par):
        s = dot(kt[h], qa[h, 0:HD])
        mo = mu_s[h]
        mu = jnp.maximum(mo, bf_round(jnp.max(s, axis=0, keepdims=True)))
        al = jnp.exp2((mo - mu) * c)
        e = jnp.exp2((s - mu) * c)
        l_s[h] = l_s[h] * al
        acc[h] = acc[h] * al
        lb_s[h] = jnp.sum(e, axis=0, keepdims=True)
        pb[par * heads + h] = e.astype(BF)
        set_shift(h, mu)

    def exact_all(b, par):
        kt[...] = jnp.swapaxes(kraw[lax.rem(b, KRAW)], 0, 1)

        def one(h, _):
            exact(h, par)
            return 0
        lax.fori_loop(0, heads, one, 0, unroll=2)

    ones = jnp.where(lax.broadcasted_iota(jnp.int32, (KB, HD), 1) == 0, 1.0, 0.0).astype(BF)
    k2 = kraw.reshape(KRAW, KB * heads, HD)
    v2 = vraw.reshape(VRAW, KB * heads, HD)

    def fast(h, par, slot):
        k = k2.at[slot][pl.ds(h, KB, stride=heads), :]
        e = jnp.exp2(dot(jnp.concatenate([k, ones], axis=1), qa[h]) * c)
        pb[par * heads + h] = e.astype(BF)
        lb_s[h] = jnp.sum(e, axis=0, keepdims=True)

    def value(h, par, slot):
        v = v2.at[slot][pl.ds(h, KB, stride=heads), :]
        l_s[h] = l_s[h] + lb_s[h]
        acc[h] = acc[h] + dot(v.T, pb[par * heads + h])

    def first(h):
        q = qa[h, 0:HD]
        s0 = jnp.where(vis, dot(kn[h], q), FLOOR)
        s1 = dot(k2.at[0][pl.ds(h, KB, stride=heads), :], q)
        mu = bf_round(jnp.maximum(jnp.max(s0, axis=0, keepdims=True), jnp.max(s1, axis=0, keepdims=True)))
        e0 = jnp.exp2((s0 - mu) * c)
        e1 = jnp.exp2((s1 - mu) * c)
        l_s[h] = jnp.sum(e0, axis=0, keepdims=True)
        lb_s[h] = jnp.sum(e1, axis=0, keepdims=True)
        pb[h] = e1.astype(BF)
        acc[h] = dot(vn[h].T, e0.astype(BF))
        set_shift(h, mu)

    @pl.when(n > 0)
    def _():
        for d in kv_copies(0):
            d.wait()
        kv_start(2)
        for h in range(heads):
            first(h)

        def block(b, _):
            for d in kv_copies(b):
                d.wait()
            kv_start(b + 2)

            @pl.when(b <= 8)
            def _():
                fetch_mid(21 + b)

            par = lax.rem(b, 2)
            ks, vs = lax.rem(b, KRAW), lax.rem(b - 1, VRAW)
            for h in range(heads):
                value(h, 1 - par, vs)
                fast(h, par, ks)

            @pl.when(jnp.logical_not(jnp.max(lb_s[...]) <= LIMIT))
            def _():
                exact_all(b, par)

            return 0

        lax.fori_loop(1, n, block, 0)
        for h in range(heads):
            value(h, lax.rem(n - 1, 2), lax.rem(n - 1, VRAW))

    def late(e, _):
        fetch_mid(e)
        return 0

    lax.fori_loop(22 + jnp.clip(n - 1, 0, 8), 30, late, 0)
    for h in range(heads):
        l = l_s[h]
        o_s[:, h * HD:(h + 1) * HD] = (acc[h] * (1.0 / l)).T.astype(BF)
        lse_s[pl.ds(h, 1)] = mu_s[h] * (HD ** -0.5) + jnp.log2(l) * log2
    lcopy = pltpu.make_async_copy(lse_s, lse_hbm, msem.at[1])
    lcopy.start()

    def o_step(i, _):
        rest = wo.shape[0] - TK
        slots = [(ready(18 + 4 * i + 2 * d), ready(19 + 4 * i + 2 * d, rest)) for d in range(2)]
        for d in range(2):
            s0, s1 = slots[d]
            cols = col(2 * i + d)
            r = dot(o_s[:, 0:TK], ring[s0]) + dot(o_s[:, TK:], ring[s1, pl.ds(0, rest)])
            h_s[:, cols] = (x_s[:, cols].astype(F32) + r).astype(BF)
        for d in range(2):
            fetch_gu(18 + 4 * i + 2 * d + RING, 2 * i + d + 2)
        return 0

    lax.fori_loop(0, 2, o_step, 0)
    a_s[...] = rms(h_s[...])

    hcopy = pltpu.make_async_copy(h_s, h_hbm, msem.at[2])
    hcopy.start()

    def t_copy(nt):
        return pltpu.make_async_copy(t_s.at[:, col(nt)], t_hbm.at[:, col(nt)], tsem.at[nt])

    def gu_pair(p):
        e = 26 + 4 * p
        slots = [ready(e + d) for d in range(4)]
        for d in range(2):
            g = dot(a_s[...], ring[slots[2 * d]])
            u = dot(a_s[...], ring[slots[2 * d + 1]])
            t_s[:, col(2 * p + d)] = (jax.nn.silu(g) * u).astype(BF)
        for d in range(2):
            t_copy(2 * p + d).start()

    def gu1(p, _):
        gu_pair(p)
        for d in range(2):
            fetch_gu(26 + 4 * p + 2 * d + RING, 2 * p + d + 6)
        return 0

    def gu2(p, _):
        gu_pair(p)
        return 0

    def drain(nt, _):
        t_copy(nt).wait()
        return 0

    lax.fori_loop(0, 5, gu1, 0)
    lax.fori_loop(5, 8, gu2, 0)
    lcopy.wait()
    hcopy.wait()
    lax.fori_loop(0, 16, drain, 0)


def down_kernel(stages, t_hbm, h_hbm, wd, y_hbm, w_s, t_s, h_s, y_s, r_s, wsem, tsem, hsem, send, recv):
    me = lax.axis_index('pipe')
    nxt = lax.rem(me + 1, stages)
    prev = lax.rem(me + stages - 1, stages)
    chunks = w_s.shape[0]
    parts = t_s.shape[0]
    width = w_s.shape[2]
    depth = t_s.shape[2]
    barrier = pltpu.get_barrier_semaphore()
    pl.semaphore_signal(barrier, inc=1, device_id={'pipe': prev}, device_id_type=pl.DeviceIdType.MESH)

    def wcopy(i, k):
        return pltpu.make_async_copy(
            wd.at[pl.ds(k * depth, depth), pl.ds(i * width, width)], w_s.at[i, pl.ds(k * depth, depth)], wsem.at[i, k])

    tcopies = [pltpu.make_async_copy(t_hbm.at[:, pl.ds(k * depth, depth)], t_s.at[k], tsem.at[k]) for k in range(parts)]
    hcopy = pltpu.make_async_copy(h_hbm, h_s, hsem)
    pieces = [(i, k) for i in range(chunks) for k in range(parts)]
    ahead = 4
    for p in range(ahead):
        if p < parts:
            tcopies[p].start()
        wcopy(*pieces[p]).start()
    hcopy.start()

    def out(i):
        cols = pl.ds(i * width, width)
        return pltpu.make_async_remote_copy(
            src_ref=y_s.at[:, cols], dst_ref=y_hbm.at[:, cols], send_sem=send.at[i], recv_sem=recv.at[i],
            device_id={'pipe': nxt}, device_id_type=pl.DeviceIdType.MESH)

    for i in range(chunks):
        cols = pl.ds(i * width, width)
        for k in range(parts):
            p = i * parts + k
            if i == 0:
                tcopies[k].wait()
            wcopy(i, k).wait()
            if p + ahead < len(pieces):
                wcopy(*pieces[p + ahead]).start()
            d = dot(t_s[k], w_s[i, pl.ds(k * depth, depth)])
            r_s[...] = d if k == 0 else r_s[...] + d
        if i == 0:
            hcopy.wait()
        y_s[:, cols] = (h_s[:, cols].astype(F32) + r_s[...]).astype(BF)
        if i == 0:
            pl.semaphore_wait(barrier, 1)
        out(i).start()
    for i in range(chunks):
        out(i).wait()


def down_call(t, h, wd, stages, width=512, parts=4):
    rows, dm = h.shape
    ff = t.shape[1]
    chunks = dm // width
    vm = pltpu.VMEM
    return pl.pallas_call(
        lambda *r: down_kernel(stages, *r),
        in_specs=[HBM] * 3,
        out_specs=pl.BlockSpec(memory_space=pltpu.VMEM),
        out_shape=jax.ShapeDtypeStruct((rows, dm), BF),
        scratch_shapes=[
            vm((chunks, ff, width), BF),
            vm((parts, rows, ff // parts), BF),
            vm((rows, dm), BF),
            vm((rows, dm), BF),
            vm((rows, width), F32),
            pltpu.SemaphoreType.DMA((chunks, parts)),
            pltpu.SemaphoreType.DMA((parts,)),
            pltpu.SemaphoreType.DMA,
            pltpu.SemaphoreType.DMA((chunks,)),
            pltpu.SemaphoreType.DMA((chunks,)),
        ],
        compiler_params=pltpu.CompilerParams(vmem_limit_bytes=48 * 2**20, collective_id=0, has_side_effects=True),
    )(t, h, wd)


def layer_call(idx, x, k, v, wq, wkv, wo, wg, wu, wd=None):
    rows, dm = x.shape
    ff = wg.shape[1]
    heads, hd = k.shape[1:]
    vm = pltpu.VMEM
    return pl.pallas_call(
        layer_kernel,
        in_specs=[SM] + [HBM] * 8,
        out_specs=[HBM] * 3,
        out_shape=[jax.ShapeDtypeStruct((rows, ff), BF), jax.ShapeDtypeStruct((rows, dm), BF), jax.ShapeDtypeStruct((heads, rows), F32)],
        scratch_shapes=[
            vm((RING, TK, TN), BF),
            vm((KRAW, KB, heads, hd), BF),
            vm((VRAW, KB, heads, hd), BF),
            vm((heads, KB, hd), BF),
            vm((heads, rows, hd), BF),
            vm((heads, rows, hd), BF),
            vm((heads, 2 * hd, rows), BF),
            vm((heads, hd, rows), F32),
            vm((2 * heads, KB, rows), BF),
            vm((heads, 1, rows), F32),
            vm((heads, 1, rows), F32),
            vm((heads, 1, rows), F32),
            vm((rows, dm), BF),
            vm((rows, dm), BF),
            vm((rows, heads * hd), BF),
            vm((rows, dm), BF),
            vm((rows, ff), BF),
            vm((heads, rows), F32),
            pltpu.SemaphoreType.DMA((RING,)),
            pltpu.SemaphoreType.DMA((2, VRAW)),
            pltpu.SemaphoreType.DMA((3,)),
            pltpu.SemaphoreType.DMA((16,)),
        ],
        compiler_params=pltpu.CompilerParams(vmem_limit_bytes=67043328),
    )(idx, x, k, v, wq, wkv, wo, wg, wu)


def solution(mesh):
    stages = mesh.shape['pipe']

    def device_step(x, idx, k, v, w_q, w_kv, w_o, w_gate, w_up, w_down):
        t, h, lse = layer_call(idx, x, k, v, w_q[0], w_kv[0], w_o[0], w_gate[0], w_up[0])
        return down_call(t, h, w_down[0], stages), lse.T

    rows_spec = P(('data', 'pipe'), None)
    cache_spec = P(('data', 'pipe'), None, None)
    stage_spec = P('pipe', None, None)
    return jax.shard_map(
        device_step,
        mesh=mesh,
        in_specs=(rows_spec, P(('data', 'pipe')), cache_spec, cache_spec) + (stage_spec,) * 6,
        out_specs=(rows_spec, rows_spec),
        check_vma=False,
    )
```

```python
import math

import jax
import jax.numpy as jnp
from jax import lax
from jax.experimental import pallas as pl
from jax.experimental.pallas import tpu as pltpu
from jax.sharding import PartitionSpec as P

BF = jnp.bfloat16
F32 = jnp.float32
HD = 128
TN = 512
TK = 2048
RING = 12
AHEAD = 4
KRAW = 3
VRAW = 4
KB = 256
FLOOR = -1e30
LIMIT = 2.0 ** 15
HBM = pl.BlockSpec(memory_space=pltpu.HBM)
SM = pl.BlockSpec(memory_space=pltpu.SMEM)


def rms(values):
    v = values.astype(F32)
    return (v * lax.rsqrt(jnp.mean(v * v, axis=-1, keepdims=True) + 1e-6)).astype(BF)


def dot(a, b):
    return jnp.dot(a, b, preferred_element_type=F32)


def layer_kernel(idx_ref, x_hbm, k_hbm, v_hbm, wq, wkv, wo, wg, wu, t_hbm, h_hbm, lse_hbm,
                 ring, kraw, vraw, kt, kn, vn, qa, acc, pa, pb, mu_s, l_s, lb_s,
                 x_s, a_s, o_s, h_s, t_s, lse_s, wsem, ksem, msem, tsem):
    n = idx_ref[0]
    rows, dm = x_s.shape
    heads = qa.shape[0]
    c = HD ** -0.5 * math.log2(math.e)
    log2 = math.log(2.0)

    def col(i, w=TN):
        return pl.ds(pl.multiple_of(i * w, w), w)

    def fetch(e, src, height=TK):
        s = lax.rem(e, RING)
        pltpu.make_async_copy(src, ring.at[s, pl.ds(0, height)], wsem.at[s]).start()

    def ready(e, height=TK):
        s = lax.rem(e, RING)
        pltpu.make_async_copy(wg.at[pl.ds(0, height), pl.ds(0, TN)], ring.at[s, pl.ds(0, height)], wsem.at[s]).wait()
        return s

    def fetch_wo(e, nt):
        fetch(e, wo.at[pl.ds(0, TK), col(nt)])
        fetch(e + 1, wo.at[pl.ds(TK, wo.shape[0] - TK), col(nt)], wo.shape[0] - TK)

    def fetch_gu(e, nt):
        fetch(e, wg.at[:, col(nt)])
        fetch(e + 1, wu.at[:, col(nt)])

    def fetch_mid(e):
        rest = wo.shape[0] - TK
        even = lax.rem(e, 2) == 0
        nt = lax.div(e - 18, 2)

        @pl.when(jnp.logical_and(e < 26, even))
        def _():
            fetch(e, wo.at[pl.ds(0, TK), col(nt)])

        @pl.when(jnp.logical_and(e < 26, jnp.logical_not(even)))
        def _():
            fetch(e, wo.at[pl.ds(TK, rest), col(nt)], rest)

        @pl.when(jnp.logical_and(e >= 26, even))
        def _():
            fetch(e, wg.at[:, col(nt - 4)])

        @pl.when(jnp.logical_and(e >= 26, jnp.logical_not(even)))
        def _():
            fetch(e, wu.at[:, col(nt - 4)])

    xcopy = pltpu.make_async_copy(x_hbm, x_s, msem.at[0])
    xcopy.start()
    for e in range(AHEAD):
        fetch(e, wq.at[:, pl.ds(e * TN, TN)])

    def kv_copies(b):
        s, t = lax.rem(b, KRAW), lax.rem(b, VRAW)
        return [
            pltpu.make_async_copy(k_hbm.at[pl.ds(b * KB, KB)], kraw.at[s], ksem.at[0, s]),
            pltpu.make_async_copy(v_hbm.at[pl.ds(b * KB, KB)], vraw.at[t], ksem.at[1, t]),
        ]

    def kv_start(b):
        @pl.when(b < n)
        def _():
            for d in kv_copies(b):
                d.start()

    qa[:, HD:] = jnp.zeros((heads, qa.shape[1] - HD, rows), BF)
    xcopy.wait()
    a_s[...] = rms(x_s[...])

    def q_step(i, _):
        @pl.when(i == 0)
        def _():
            for d in range(AHEAD, 6):
                fetch(d, wq.at[:, pl.ds(d * TN, TN)])

        @pl.when(i > 0)
        def _():
            for d in range(2):
                fetch(2 * i + AHEAD + d, wkv.at[:, col(2 * i + AHEAD + d - 6)])

        for d in range(2):
            e = 2 * i + d
            s = ready(e)
            t = dot(a_s[...], ring[s]).astype(BF)
            for j in range(4):
                qa[4 * e + j, 0:HD] = t[:, j * HD:(j + 1) * HD].T
        return 0

    lax.fori_loop(0, 3, q_step, 0)

    def fetch_kv(e):
        for d in range(2):
            fetch(e + d, wkv.at[:, col(e + d - 6)])

    def kv_tiles(e, dst, base):
        for d in range(2):
            s = ready(e + d)
            t = dot(a_s[...], ring[s]).astype(BF)
            for j in range(4):
                dst[base + 4 * d + j] = t[:, j * HD:(j + 1) * HD]

    def k_step(i, _):
        e = 6 + 2 * i
        fetch_kv(e + AHEAD)
        kv_tiles(e, kn, 8 * i)
        return 0

    lax.fori_loop(0, 3, k_step, 0)
    fetch_kv(12 + AHEAD)
    kv_start(0)
    kv_start(1)
    kv_tiles(12, vn, 0)

    def v_step(i, _):
        e = 14 + 2 * i
        fetch_wo(e + AHEAD, i)
        kv_tiles(e, vn, 8 * i + 8)
        return 0

    lax.fori_loop(0, 2, v_step, 0)

    def bf_round(v):
        return v.astype(BF).astype(F32)

    def set_shift(h, mu):
        mu_s[h] = mu
        first = lax.broadcasted_iota(jnp.int32, (16, rows), 0) == 0
        qa[h, HD:HD + 16] = jnp.where(first, -mu, 0.0).astype(BF)

    vis = lax.broadcasted_iota(jnp.int32, (KB, rows), 0) <= lax.broadcasted_iota(jnp.int32, (KB, rows), 1)

    def local(h, _):
        s = jnp.where(vis, dot(kn[h], qa[h, 0:HD]), FLOOR)
        mu = bf_round(jnp.max(s, axis=0, keepdims=True))
        e = jnp.exp2((s - mu) * c)
        l_s[h] = jnp.sum(e, axis=0, keepdims=True)
        acc[h] = dot(vn[h].T, e.astype(BF))
        set_shift(h, mu)
        return 0

    @pl.when(n == 0)
    def _():
        lax.fori_loop(0, heads, local, 0, unroll=4)

    def exact(h, cur):
        s = dot(kt[h], qa[h, 0:HD])
        mo = mu_s[h]
        mu = jnp.maximum(mo, bf_round(jnp.max(s, axis=0, keepdims=True)))
        al = jnp.exp2((mo - mu) * c)
        e = jnp.exp2((s - mu) * c)
        l_s[h] = l_s[h] * al
        acc[h] = acc[h] * al
        lb_s[h] = jnp.sum(e, axis=0, keepdims=True)
        cur[h] = e.astype(BF)
        set_shift(h, mu)

    def exact_all(b, cur):
        kt[...] = jnp.swapaxes(kraw[lax.rem(b, KRAW)], 0, 1)

        def one(h, _):
            exact(h, cur)
            return 0
        lax.fori_loop(0, heads, one, 0, unroll=2)

    ones = jnp.where(lax.broadcasted_iota(jnp.int32, (KB, HD), 1) == 0, 1.0, 0.0).astype(BF)
    k2 = kraw.reshape(KRAW, KB * heads, HD)
    v2 = vraw.reshape(VRAW, KB * heads, HD)

    def fast(h, cur, slot):
        k = k2.at[slot][pl.ds(h, KB, stride=heads), :]
        e = jnp.exp2(dot(jnp.concatenate([k, ones], axis=1), qa[h]) * c)
        cur[h] = e.astype(BF)
        lb_s[h] = jnp.sum(e, axis=0, keepdims=True)

    def value(h, prev, slot):
        v = v2.at[slot][pl.ds(h, KB, stride=heads), :]
        l_s[h] = l_s[h] + lb_s[h]
        acc[h] = acc[h] + dot(v.T, prev[h])

    def first(h):
        q = qa[h, 0:HD]
        s0 = jnp.where(vis, dot(kn[h], q), FLOOR)
        s1 = dot(k2.at[0][pl.ds(h, KB, stride=heads), :], q)
        mu = bf_round(jnp.maximum(jnp.max(s0, axis=0, keepdims=True), jnp.max(s1, axis=0, keepdims=True)))
        e0 = jnp.exp2((s0 - mu) * c)
        e1 = jnp.exp2((s1 - mu) * c)
        l_s[h] = jnp.sum(e0, axis=0, keepdims=True)
        lb_s[h] = jnp.sum(e1, axis=0, keepdims=True)
        pa[h] = e1.astype(BF)
        acc[h] = dot(vn[h].T, e0.astype(BF))
        set_shift(h, mu)

    @pl.when(n > 0)
    def _():
        for d in kv_copies(0):
            d.wait()
        kv_start(2)
        for h in range(heads):
            first(h)

        def block(b, prev, cur):
            for d in kv_copies(b):
                d.wait()
            kv_start(b + 2)

            @pl.when(b <= 8)
            def _():
                fetch_mid(21 + b)

            ks, vs = lax.rem(b, KRAW), lax.rem(b - 1, VRAW)
            for h in range(heads):
                value(h, prev, vs)
                fast(h, cur, ks)

            @pl.when(jnp.logical_not(jnp.max(lb_s[...]) <= LIMIT))
            def _():
                exact_all(b, cur)

        def two(i, _):
            b = 2 * i + 1
            block(b, pa, pb)

            @pl.when(b + 1 < n)
            def _():
                block(b + 1, pb, pa)

            return 0

        lax.fori_loop(0, lax.div(n, 2), two, 0)

        @pl.when(lax.rem(n, 2) == 1)
        def _():
            for h in range(heads):
                value(h, pa, lax.rem(n - 1, VRAW))

        @pl.when(lax.rem(n, 2) == 0)
        def _():
            for h in range(heads):
                value(h, pb, lax.rem(n - 1, VRAW))

    def late(e, _):
        fetch_mid(e)
        return 0

    lax.fori_loop(22 + jnp.clip(n - 1, 0, 8), 30, late, 0)
    for h in range(heads):
        l = l_s[h]
        o_s[:, h * HD:(h + 1) * HD] = (acc[h] * (1.0 / l)).T.astype(BF)
        lse_s[pl.ds(h, 1)] = mu_s[h] * (HD ** -0.5) + jnp.log2(l) * log2
    lcopy = pltpu.make_async_copy(lse_s, lse_hbm, msem.at[1])
    lcopy.start()

    def o_step(i, _):
        rest = wo.shape[0] - TK
        slots = [(ready(18 + 4 * i + 2 * d), ready(19 + 4 * i + 2 * d, rest)) for d in range(2)]
        for d in range(2):
            s0, s1 = slots[d]
            cols = col(2 * i + d)
            r = dot(o_s[:, 0:TK], ring[s0]) + dot(o_s[:, TK:], ring[s1, pl.ds(0, rest)])
            h_s[:, cols] = (x_s[:, cols].astype(F32) + r).astype(BF)
        for d in range(2):
            fetch_gu(18 + 4 * i + 2 * d + RING, 2 * i + d + 2)
        return 0

    lax.fori_loop(0, 2, o_step, 0)
    a_s[...] = rms(h_s[...])

    hcopy = pltpu.make_async_copy(h_s, h_hbm, msem.at[2])
    hcopy.start()

    def t_copy(nt):
        return pltpu.make_async_copy(t_s.at[:, col(nt)], t_hbm.at[:, col(nt)], tsem.at[nt])

    def gu_pair(p):
        e = 26 + 4 * p
        slots = [ready(e + d) for d in range(4)]
        for d in range(2):
            g = dot(a_s[...], ring[slots[2 * d]])
            u = dot(a_s[...], ring[slots[2 * d + 1]])
            t_s[:, col(2 * p + d)] = (jax.nn.silu(g) * u).astype(BF)
        for d in range(2):
            t_copy(2 * p + d).start()

    def gu1(p, _):
        gu_pair(p)
        for d in range(2):
            fetch_gu(26 + 4 * p + 2 * d + RING, 2 * p + d + 6)
        return 0

    def gu2(p, _):
        gu_pair(p)
        return 0

    def drain(nt, _):
        t_copy(nt).wait()
        return 0

    lax.fori_loop(0, 5, gu1, 0)
    lax.fori_loop(5, 8, gu2, 0)
    lcopy.wait()
    hcopy.wait()
    lax.fori_loop(0, 16, drain, 0)


def down_kernel(stages, t_hbm, h_hbm, wd, y_hbm, w_s, t_s, h_s, y_s, r_s, wsem, tsem, hsem, send, recv):
    me = lax.axis_index('pipe')
    nxt = lax.rem(me + 1, stages)
    prev = lax.rem(me + stages - 1, stages)
    chunks = w_s.shape[0]
    parts = t_s.shape[0]
    width = w_s.shape[2]
    depth = t_s.shape[2]
    barrier = pltpu.get_barrier_semaphore()
    pl.semaphore_signal(barrier, inc=1, device_id={'pipe': prev}, device_id_type=pl.DeviceIdType.MESH)

    def wcopy(i, k):
        return pltpu.make_async_copy(
            wd.at[pl.ds(k * depth, depth), pl.ds(i * width, width)], w_s.at[i, pl.ds(k * depth, depth)], wsem.at[i, k])

    tcopies = [pltpu.make_async_copy(t_hbm.at[:, pl.ds(k * depth, depth)], t_s.at[k], tsem.at[k]) for k in range(parts)]
    hcopy = pltpu.make_async_copy(h_hbm, h_s, hsem)
    pieces = [(i, k) for i in range(chunks) for k in range(parts)]
    ahead = 4
    for p in range(ahead):
        if p < parts:
            tcopies[p].start()
        wcopy(*pieces[p]).start()
    hcopy.start()

    def out(i):
        cols = pl.ds(i * width, width)
        return pltpu.make_async_remote_copy(
            src_ref=y_s.at[:, cols], dst_ref=y_hbm.at[:, cols], send_sem=send.at[i], recv_sem=recv.at[i],
            device_id={'pipe': nxt}, device_id_type=pl.DeviceIdType.MESH)

    for i in range(chunks):
        cols = pl.ds(i * width, width)
        for k in range(parts):
            p = i * parts + k
            if i == 0:
                tcopies[k].wait()
            wcopy(i, k).wait()
            if p + ahead < len(pieces):
                wcopy(*pieces[p + ahead]).start()
            d = dot(t_s[k], w_s[i, pl.ds(k * depth, depth)])
            r_s[...] = d if k == 0 else r_s[...] + d
        if i == 0:
            hcopy.wait()
        y_s[:, cols] = (h_s[:, cols].astype(F32) + r_s[...]).astype(BF)
        if i == 0:
            pl.semaphore_wait(barrier, 1)
        out(i).start()
    for i in range(chunks):
        out(i).wait()


def down_call(t, h, wd, stages, width=512, parts=4):
    rows, dm = h.shape
    ff = t.shape[1]
    chunks = dm // width
    vm = pltpu.VMEM
    return pl.pallas_call(
        lambda *r: down_kernel(stages, *r),
        in_specs=[HBM] * 3,
        out_specs=pl.BlockSpec(memory_space=pltpu.VMEM),
        out_shape=jax.ShapeDtypeStruct((rows, dm), BF),
        scratch_shapes=[
            vm((chunks, ff, width), BF),
            vm((parts, rows, ff // parts), BF),
            vm((rows, dm), BF),
            vm((rows, dm), BF),
            vm((rows, width), F32),
            pltpu.SemaphoreType.DMA((chunks, parts)),
            pltpu.SemaphoreType.DMA((parts,)),
            pltpu.SemaphoreType.DMA,
            pltpu.SemaphoreType.DMA((chunks,)),
            pltpu.SemaphoreType.DMA((chunks,)),
        ],
        compiler_params=pltpu.CompilerParams(vmem_limit_bytes=48 * 2**20, collective_id=0, has_side_effects=True),
    )(t, h, wd)


def layer_call(idx, x, k, v, wq, wkv, wo, wg, wu, wd=None):
    rows, dm = x.shape
    ff = wg.shape[1]
    heads, hd = k.shape[1:]
    vm = pltpu.VMEM
    return pl.pallas_call(
        layer_kernel,
        in_specs=[SM] + [HBM] * 8,
        out_specs=[HBM] * 3,
        out_shape=[jax.ShapeDtypeStruct((rows, ff), BF), jax.ShapeDtypeStruct((rows, dm), BF), jax.ShapeDtypeStruct((heads, rows), F32)],
        scratch_shapes=[
            vm((RING, TK, TN), BF),
            vm((KRAW, KB, heads, hd), BF),
            vm((VRAW, KB, heads, hd), BF),
            vm((heads, KB, hd), BF),
            vm((heads, rows, hd), BF),
            vm((heads, rows, hd), BF),
            vm((heads, 2 * hd, rows), BF),
            vm((heads, hd, rows), F32),
            vm((heads, KB, rows), BF),
            vm((heads, KB, rows), BF),
            vm((heads, 1, rows), F32),
            vm((heads, 1, rows), F32),
            vm((heads, 1, rows), F32),
            vm((rows, dm), BF),
            vm((rows, dm), BF),
            vm((rows, heads * hd), BF),
            vm((rows, dm), BF),
            vm((rows, ff), BF),
            vm((heads, rows), F32),
            pltpu.SemaphoreType.DMA((RING,)),
            pltpu.SemaphoreType.DMA((2, VRAW)),
            pltpu.SemaphoreType.DMA((3,)),
            pltpu.SemaphoreType.DMA((16,)),
        ],
        compiler_params=pltpu.CompilerParams(vmem_limit_bytes=67043328),
    )(idx, x, k, v, wq, wkv, wo, wg, wu)


def solution(mesh):
    stages = mesh.shape['pipe']

    def device_step(x, idx, k, v, w_q, w_kv, w_o, w_gate, w_up, w_down):
        t, h, lse = layer_call(idx, x, k, v, w_q[0], w_kv[0], w_o[0], w_gate[0], w_up[0])
        return down_call(t, h, w_down[0], stages), lse.T

    rows_spec = P(('data', 'pipe'), None)
    cache_spec = P(('data', 'pipe'), None, None)
    stage_spec = P('pipe', None, None)
    return jax.shard_map(
        device_step,
        mesh=mesh,
        in_specs=(rows_spec, P(('data', 'pipe')), cache_spec, cache_spec) + (stage_spec,) * 6,
        out_specs=(rows_spec, rows_spec),
        check_vma=False,
    )
```

```python
import math

import jax
import jax.numpy as jnp
from jax import lax
from jax.experimental import pallas as pl
from jax.experimental.pallas import tpu as pltpu
from jax.sharding import PartitionSpec as P

BF = jnp.bfloat16
F32 = jnp.float32
HD = 128
TN = 512
TK = 2048
RING = 12
AHEAD = 4
KRAW = 3
VRAW = 4
KB = 256
FLOOR = -1e30
LIMIT = 2.0 ** 15
HBM = pl.BlockSpec(memory_space=pltpu.HBM)
SM = pl.BlockSpec(memory_space=pltpu.SMEM)


def rms(values):
    v = values.astype(F32)
    return (v * lax.rsqrt(jnp.mean(v * v, axis=-1, keepdims=True) + 1e-6)).astype(BF)


def dot(a, b):
    return jnp.dot(a, b, preferred_element_type=F32)


def layer_kernel(idx_ref, x_hbm, k_hbm, v_hbm, wq, wkv, wo, wg, wu, t_hbm, h_hbm, lse_hbm,
                 ring, kraw, vraw, kt, kn, vn, qa, acc, pa, pb, mu_s, l_s, lb_s,
                 x_s, a_s, o_s, h_s, t_s, lse_s, wsem, ksem, msem, tsem):
    n = idx_ref[0]
    rows, dm = x_s.shape
    heads = qa.shape[0]
    c = HD ** -0.5 * math.log2(math.e)
    log2 = math.log(2.0)

    def col(i, w=TN):
        return pl.ds(pl.multiple_of(i * w, w), w)

    def fetch(e, src, height=TK):
        s = lax.rem(e, RING)
        pltpu.make_async_copy(src, ring.at[s, pl.ds(0, height)], wsem.at[s]).start()

    def ready(e, height=TK):
        s = lax.rem(e, RING)
        pltpu.make_async_copy(wg.at[pl.ds(0, height), pl.ds(0, TN)], ring.at[s, pl.ds(0, height)], wsem.at[s]).wait()
        return s

    def fetch_wo(e, nt):
        fetch(e, wo.at[pl.ds(0, TK), col(nt)])
        fetch(e + 1, wo.at[pl.ds(TK, wo.shape[0] - TK), col(nt)], wo.shape[0] - TK)

    def fetch_gu(e, nt):
        fetch(e, wg.at[:, col(nt)])
        fetch(e + 1, wu.at[:, col(nt)])

    def fetch_mid(e):
        rest = wo.shape[0] - TK
        even = lax.rem(e, 2) == 0
        nt = lax.div(e - 18, 2)

        @pl.when(jnp.logical_and(e < 26, even))
        def _():
            fetch(e, wo.at[pl.ds(0, TK), col(nt)])

        @pl.when(jnp.logical_and(e < 26, jnp.logical_not(even)))
        def _():
            fetch(e, wo.at[pl.ds(TK, rest), col(nt)], rest)

        @pl.when(jnp.logical_and(e >= 26, even))
        def _():
            fetch(e, wg.at[:, col(nt - 4)])

        @pl.when(jnp.logical_and(e >= 26, jnp.logical_not(even)))
        def _():
            fetch(e, wu.at[:, col(nt - 4)])

    xcopy = pltpu.make_async_copy(x_hbm, x_s, msem.at[0])
    xcopy.start()
    for e in range(AHEAD):
        fetch(e, wq.at[:, pl.ds(e * TN, TN)])

    def kv_copies(b):
        s, t = lax.rem(b, KRAW), lax.rem(b, VRAW)
        return [
            pltpu.make_async_copy(k_hbm.at[pl.ds(b * KB, KB)], kraw.at[s], ksem.at[0, s]),
            pltpu.make_async_copy(v_hbm.at[pl.ds(b * KB, KB)], vraw.at[t], ksem.at[1, t]),
        ]

    def kv_start(b):
        @pl.when(b < n)
        def _():
            for d in kv_copies(b):
                d.start()

    qa[:, HD:] = jnp.zeros((heads, qa.shape[1] - HD, rows), BF)
    xcopy.wait()
    a_s[...] = rms(x_s[...])

    def q_step(i, _):
        @pl.when(i == 0)
        def _():
            for d in range(AHEAD, 6):
                fetch(d, wq.at[:, pl.ds(d * TN, TN)])

        @pl.when(i > 0)
        def _():
            for d in range(2):
                fetch(2 * i + AHEAD + d, wkv.at[:, col(2 * i + AHEAD + d - 6)])

        for d in range(2):
            e = 2 * i + d
            s = ready(e)
            t = dot(a_s[...], ring[s]).astype(BF)
            for j in range(4):
                qa[4 * e + j, 0:HD] = t[:, j * HD:(j + 1) * HD].T
        return 0

    lax.fori_loop(0, 3, q_step, 0)

    def fetch_kv(e):
        for d in range(2):
            fetch(e + d, wkv.at[:, col(e + d - 6)])

    def kv_tiles(e, dst, base):
        for d in range(2):
            s = ready(e + d)
            t = dot(a_s[...], ring[s]).astype(BF)
            for j in range(4):
                dst[base + 4 * d + j] = t[:, j * HD:(j + 1) * HD]

    def k_step(i, _):
        e = 6 + 2 * i
        fetch_kv(e + AHEAD)
        kv_tiles(e, kn, 8 * i)
        return 0

    lax.fori_loop(0, 3, k_step, 0)
    fetch_kv(12 + AHEAD)
    kv_start(0)
    kv_start(1)
    kv_tiles(12, vn, 0)

    def v_step(i, _):
        e = 14 + 2 * i
        fetch_wo(e + AHEAD, i)
        kv_tiles(e, vn, 8 * i + 8)
        return 0

    lax.fori_loop(0, 2, v_step, 0)

    def bf_round(v):
        return v.astype(BF).astype(F32)

    def set_shift(h, mu):
        mu_s[h] = mu
        first = lax.broadcasted_iota(jnp.int32, (16, rows), 0) == 0
        qa[h, HD:HD + 16] = jnp.where(first, -mu, 0.0).astype(BF)

    vis = lax.broadcasted_iota(jnp.int32, (KB, rows), 0) <= lax.broadcasted_iota(jnp.int32, (KB, rows), 1)

    def local(h, _):
        s = jnp.where(vis, dot(kn[h], qa[h, 0:HD]), FLOOR)
        mu = bf_round(jnp.max(s, axis=0, keepdims=True))
        e = jnp.exp2((s - mu) * c)
        l_s[h] = jnp.sum(e, axis=0, keepdims=True)
        acc[h] = dot(vn[h].T, e.astype(BF))
        set_shift(h, mu)
        return 0

    @pl.when(n == 0)
    def _():
        lax.fori_loop(0, heads, local, 0, unroll=4)

    def exact(h, cur):
        s = dot(kt[h], qa[h, 0:HD])
        mo = mu_s[h]
        mu = jnp.maximum(mo, bf_round(jnp.max(s, axis=0, keepdims=True)))
        al = jnp.exp2((mo - mu) * c)
        e = jnp.exp2((s - mu) * c)
        l_s[h] = l_s[h] * al
        acc[h] = acc[h] * al
        lb_s[h] = jnp.sum(e, axis=0, keepdims=True)
        cur[h] = e.astype(BF)
        set_shift(h, mu)

    def exact_all(b, cur):
        kt[...] = jnp.swapaxes(kraw[lax.rem(b, KRAW)], 0, 1)

        def one(h, _):
            exact(h, cur)
            return 0
        lax.fori_loop(0, heads, one, 0, unroll=2)

    ones = jnp.where(lax.broadcasted_iota(jnp.int32, (KB, HD), 1) == 0, 1.0, 0.0).astype(BF)
    k2 = kraw.reshape(KRAW, KB * heads, HD)
    v2 = vraw.reshape(VRAW, KB * heads, HD)

    def fast(h, cur, slot):
        k = k2.at[slot][pl.ds(h, KB, stride=heads), :]
        e = jnp.exp2(dot(jnp.concatenate([k, ones], axis=1), qa[h]) * c)
        cur[h] = e.astype(BF)
        lb_s[h] = jnp.sum(e, axis=0, keepdims=True)

    def value(h, prev, slot):
        v = v2.at[slot][pl.ds(h, KB, stride=heads), :]
        l_s[h] = l_s[h] + lb_s[h]
        acc[h] = acc[h] + dot(v.T, prev[h])

    def first(h):
        q = qa[h, 0:HD]
        s0 = jnp.where(vis, dot(kn[h], q), FLOOR)
        s1 = dot(k2.at[0][pl.ds(h, KB, stride=heads), :], q)
        mu = bf_round(jnp.maximum(jnp.max(s0, axis=0, keepdims=True), jnp.max(s1, axis=0, keepdims=True)))
        e0 = jnp.exp2((s0 - mu) * c)
        e1 = jnp.exp2((s1 - mu) * c)
        l_s[h] = jnp.sum(e0, axis=0, keepdims=True)
        lb_s[h] = jnp.sum(e1, axis=0, keepdims=True)
        pa[h] = e1.astype(BF)
        acc[h] = dot(vn[h].T, e0.astype(BF))
        set_shift(h, mu)

    @pl.when(n > 0)
    def _():
        for d in kv_copies(0):
            d.wait()
        kv_start(2)
        for h in range(heads):
            first(h)

        def block(b, prev, cur):
            for d in kv_copies(b):
                d.wait()
            kv_start(b + 2)

            @pl.when(b <= 8)
            def _():
                fetch_mid(21 + b)

            ks, vs = lax.rem(b, KRAW), lax.rem(b - 1, VRAW)
            for h in range(heads):
                value(h, prev, vs)
                fast(h, cur, ks)

            @pl.when(jnp.logical_not(jnp.max(lb_s[...]) <= LIMIT))
            def _():
                exact_all(b, cur)

        def two(i, _):
            b = 2 * i + 1
            block(b, pa, pb)

            @pl.when(b + 1 < n)
            def _():
                block(b + 1, pb, pa)

            return 0

        lax.fori_loop(0, lax.div(n, 2), two, 0)

        @pl.when(lax.rem(n, 2) == 1)
        def _():
            for h in range(heads):
                value(h, pa, lax.rem(n - 1, VRAW))

        @pl.when(lax.rem(n, 2) == 0)
        def _():
            for h in range(heads):
                value(h, pb, lax.rem(n - 1, VRAW))

    def late(e, _):
        fetch_mid(e)
        return 0

    lax.fori_loop(22 + jnp.clip(n - 1, 0, 8), 30, late, 0)
    for h in range(heads):
        l = l_s[h]
        o_s[:, h * HD:(h + 1) * HD] = (acc[h] * (1.0 / l)).T.astype(BF)
        lse_s[pl.ds(h, 1)] = mu_s[h] * (HD ** -0.5) + jnp.log2(l) * log2
    lcopy = pltpu.make_async_copy(lse_s, lse_hbm, msem.at[1])
    lcopy.start()

    def o_step(i, _):
        rest = wo.shape[0] - TK
        slots = [(ready(18 + 4 * i + 2 * d), ready(19 + 4 * i + 2 * d, rest)) for d in range(2)]
        for d in range(2):
            s0, s1 = slots[d]
            cols = col(2 * i + d)
            r = dot(o_s[:, 0:TK], ring[s0]) + dot(o_s[:, TK:], ring[s1, pl.ds(0, rest)])
            h_s[:, cols] = (x_s[:, cols].astype(F32) + r).astype(BF)
        for d in range(2):
            fetch_gu(18 + 4 * i + 2 * d + RING, 2 * i + d + 2)
        return 0

    lax.fori_loop(0, 2, o_step, 0)
    a_s[...] = rms(h_s[...])

    hcopy = pltpu.make_async_copy(h_s, h_hbm, msem.at[2])
    hcopy.start()

    def t_copy(nt):
        return pltpu.make_async_copy(t_s.at[:, col(nt)], t_hbm.at[:, col(nt)], tsem.at[nt])

    def gu_pair(p):
        e = 26 + 4 * p
        slots = [ready(e + d) for d in range(4)]
        for d in range(2):
            g = dot(a_s[...], ring[slots[2 * d]])
            u = dot(a_s[...], ring[slots[2 * d + 1]])
            t_s[:, col(2 * p + d)] = (jax.nn.silu(g) * u).astype(BF)
        for d in range(2):
            t_copy(2 * p + d).start()

    def gu1(p, _):
        gu_pair(p)
        for d in range(2):
            fetch_gu(26 + 4 * p + 2 * d + RING, 2 * p + d + 6)
        return 0

    def gu2(p, _):
        gu_pair(p)
        return 0

    def drain(nt, _):
        t_copy(nt).wait()
        return 0

    lax.fori_loop(0, 5, gu1, 0)
    lax.fori_loop(5, 8, gu2, 0)
    lcopy.wait()
    hcopy.wait()
    lax.fori_loop(0, 16, drain, 0)


def down_kernel(stages, t_hbm, h_hbm, wd, y_hbm, w_s, t_s, h_s, y_s, r_s, wsem, tsem, hsem, send, recv):
    me = lax.axis_index('pipe')
    nxt = lax.rem(me + 1, stages)
    prev = lax.rem(me + stages - 1, stages)
    chunks = w_s.shape[0]
    parts = t_s.shape[0]
    width = w_s.shape[2]
    depth = t_s.shape[2]
    barrier = pltpu.get_barrier_semaphore()
    pl.semaphore_signal(barrier, inc=1, device_id={'pipe': prev}, device_id_type=pl.DeviceIdType.MESH)

    def wcopy(i, k):
        return pltpu.make_async_copy(
            wd.at[pl.ds(k * depth, depth), pl.ds(i * width, width)], w_s.at[i, pl.ds(k * depth, depth)], wsem.at[i, k])

    tcopies = [pltpu.make_async_copy(t_hbm.at[:, pl.ds(k * depth, depth)], t_s.at[k], tsem.at[k]) for k in range(parts)]
    hcopy = pltpu.make_async_copy(h_hbm, h_s, hsem)
    pieces = [(i, k) for i in range(chunks) for k in range(parts)]
    ahead = 4
    for p in range(ahead):
        if p < parts:
            tcopies[p].start()
        wcopy(*pieces[p]).start()
    hcopy.start()

    def out(i):
        cols = pl.ds(i * width, width)
        return pltpu.make_async_remote_copy(
            src_ref=y_s.at[:, cols], dst_ref=y_hbm.at[:, cols], send_sem=send.at[i], recv_sem=recv.at[i],
            device_id={'pipe': nxt}, device_id_type=pl.DeviceIdType.MESH)

    for i in range(chunks):
        cols = pl.ds(i * width, width)
        for k in range(parts):
            p = i * parts + k
            if i == 0:
                tcopies[k].wait()
            wcopy(i, k).wait()
            if p + ahead < len(pieces):
                wcopy(*pieces[p + ahead]).start()
            d = dot(t_s[k], w_s[i, pl.ds(k * depth, depth)])
            r_s[...] = d if k == 0 else r_s[...] + d
        if i == 0:
            hcopy.wait()
        y_s[:, cols] = (h_s[:, cols].astype(F32) + r_s[...]).astype(BF)
        if i == 0:
            pl.semaphore_wait(barrier, 1)
        out(i).start()
    for i in range(chunks):
        out(i).wait()


def down_call(t, h, wd, stages, width=512, parts=4):
    rows, dm = h.shape
    ff = t.shape[1]
    chunks = dm // width
    vm = pltpu.VMEM
    return pl.pallas_call(
        lambda *r: down_kernel(stages, *r),
        in_specs=[HBM] * 3,
        out_specs=pl.BlockSpec(memory_space=pltpu.VMEM),
        out_shape=jax.ShapeDtypeStruct((rows, dm), BF),
        scratch_shapes=[
            vm((chunks, ff, width), BF),
            vm((parts, rows, ff // parts), BF),
            vm((rows, dm), BF),
            vm((rows, dm), BF),
            vm((rows, width), F32),
            pltpu.SemaphoreType.DMA((chunks, parts)),
            pltpu.SemaphoreType.DMA((parts,)),
            pltpu.SemaphoreType.DMA,
            pltpu.SemaphoreType.DMA((chunks,)),
            pltpu.SemaphoreType.DMA((chunks,)),
        ],
        compiler_params=pltpu.CompilerParams(vmem_limit_bytes=48 * 2**20, collective_id=0, has_side_effects=True),
    )(t, pltpu.with_memory_space_constraint(h, pltpu.HBM), wd)


def layer_call(idx, x, k, v, wq, wkv, wo, wg, wu, wd=None):
    rows, dm = x.shape
    ff = wg.shape[1]
    heads, hd = k.shape[1:]
    vm = pltpu.VMEM
    return pl.pallas_call(
        layer_kernel,
        in_specs=[SM] + [HBM] * 8,
        out_specs=[HBM] * 3,
        out_shape=[jax.ShapeDtypeStruct((rows, ff), BF), jax.ShapeDtypeStruct((rows, dm), BF), jax.ShapeDtypeStruct((heads, rows), F32)],
        scratch_shapes=[
            vm((RING, TK, TN), BF),
            vm((KRAW, KB, heads, hd), BF),
            vm((VRAW, KB, heads, hd), BF),
            vm((heads, KB, hd), BF),
            vm((heads, rows, hd), BF),
            vm((heads, rows, hd), BF),
            vm((heads, 2 * hd, rows), BF),
            vm((heads, hd, rows), F32),
            vm((heads, KB, rows), BF),
            vm((heads, KB, rows), BF),
            vm((heads, 1, rows), F32),
            vm((heads, 1, rows), F32),
            vm((heads, 1, rows), F32),
            vm((rows, dm), BF),
            vm((rows, dm), BF),
            vm((rows, heads * hd), BF),
            vm((rows, dm), BF),
            vm((rows, ff), BF),
            vm((heads, rows), F32),
            pltpu.SemaphoreType.DMA((RING,)),
            pltpu.SemaphoreType.DMA((2, VRAW)),
            pltpu.SemaphoreType.DMA((3,)),
            pltpu.SemaphoreType.DMA((16,)),
        ],
        compiler_params=pltpu.CompilerParams(vmem_limit_bytes=67043328),
    )(idx, x, k, v, wq, wkv, wo, wg, wu)


def solution(mesh):
    stages = mesh.shape['pipe']

    def device_step(x, idx, k, v, w_q, w_kv, w_o, w_gate, w_up, w_down):
        t, h, lse = layer_call(idx, x, k, v, w_q[0], w_kv[0], w_o[0], w_gate[0], w_up[0])
        return down_call(t, h, w_down[0], stages), lse.T

    rows_spec = P(('data', 'pipe'), None)
    cache_spec = P(('data', 'pipe'), None, None)
    stage_spec = P('pipe', None, None)
    return jax.shard_map(
        device_step,
        mesh=mesh,
        in_specs=(rows_spec, P(('data', 'pipe')), cache_spec, cache_spec) + (stage_spec,) * 6,
        out_specs=(rows_spec, rows_spec),
        check_vma=False,
    )
```
